32 devices in a mesh: gx: 2 (over y), gy: 4 (over x, core), gz: 4 (over z).
Axes of the slice: x: 2, y: 2, z: 4, core: 2. Of those that a mesh axis runs over, the one named last changes fastest.
Arguments:
- volume: float32 [16, 64, 512], P(('gx', 'gy'), None, 'gz'), may hold values from 0 to 1
- levels: int32 [4], replicated, may hold values from 0 to 255
Outputs:
- labelling: float32 [4, 16, 64, 512], P(None, 'gx', 'gy', 'gz')
- centers: float32 [4], replicated
The draws below stay inside these ranges and needn't reach their ends.
All inputs are finite; a program needn't handle non-finite values.
Results may differ from the reference program's by a relative error of at most 0.0001.
Values sent between devices are 32-bit elements; how exact they have to be, the bound alone decides.
No kernel may reach another device: no remote copies, remote signals or barrier semaphores. Data moves between devices by JAX's collectives and lax.ppermute only.
A program may use at most 64 MiB of HBM per device.

```python
import jax
import jax.numpy as jnp
from jax import lax

LABELS = 4
ITERS = 2
NX = 16
NY = 64
NZ = 512


def with_ends(result, key, least, high):
    longest = result.shape.index(max(result.shape))
    spots = []
    for shift in (0, 1):
        where = [jax.random.randint(jax.random.fold_in(key, axis), (), 0, length) for axis, length in enumerate(result.shape)]
        where[longest] = (where[longest] + shift) % result.shape[longest]
        spots.append(tuple(where))
    return result.at[spots[0]].set(least).at[spots[1]].set(high)


def steps_of(rng, shape, pieces, least, largest):
    level, own = 1.0, jax.random.fold_in(rng, 6)
    for dim, parts in pieces:
        draws = jnp.exp(jax.random.uniform(jax.random.fold_in(own, dim), (parts,), jnp.float32, least / len(pieces), largest / len(pieces)))
        level = level * jnp.repeat(draws, shape[dim] // parts).reshape([-1 if axis == dim else 1 for axis in range(len(shape))])
    return level


def setup_inputs(seed: int = 0) -> dict:
    key_of = jax.random.split(jax.random.key(seed), 3)
    return {
        "volume": jnp.clip(1.0 * jax.random.uniform(key_of[0], (NX, NY, NZ), jnp.float32) ** steps_of(key_of[0], (NX, NY, NZ), ((0, 8), (2, 4)), -0.2, 0.2), 0.0, 1.0),
        "levels": with_ends(jax.random.randint(key_of[1], (LABELS,), 0, 256), jax.random.fold_in(key_of[1], 1), 0, 255).astype(jnp.int32),
    }


tau_step = 0.25
sigma_step = 0.25
smooth_weight = 0.5
prior_weight = 1.0

def project_simplex(values):
    how_many = values.shape[0]
    threshold = None
    for subset in range(1, 1 << how_many):
        members = [label_index for label_index in range(how_many) if subset >> label_index & 1]
        summed = values[members[0]]
        for label_index in members[1:]:
            summed = summed + values[label_index]
        candidate = (summed - 1.0) / float(len(members))
        threshold = candidate if threshold is None else jnp.maximum(threshold, candidate)
    return jnp.maximum(values - threshold[None], 0.0)

def forward(values, axis):
    extent = values.shape[axis]
    return jnp.diff(values, axis=axis, append=lax.slice_in_dim(values, extent - 1, extent, axis=axis))

def backward(values, axis):
    return jnp.diff(values, axis=axis, prepend=jnp.float32(0.0))

def reference(volume, levels):
    base_levels = levels.astype(jnp.float32) / 255.0
    centers = base_levels
    starting = (volume[None] - base_levels[:, None, None, None]) ** 2
    labelling = project_simplex(1.0 / LABELS - tau_step * starting)
    smoothed = labelling
    dual_field = [[jnp.zeros((NX, NY, NZ), jnp.float32) for axis in range(3)] for label_index in range(LABELS)]
    for iteration in range(ITERS):
        divergences = []
        renewed = []
        for label_index in range(LABELS):
            stepped = [dual_field[label_index][axis] + sigma_step * forward(smoothed[label_index], axis) for axis in range(3)]
            length = jnp.sqrt(stepped[0] * stepped[0] + stepped[1] * stepped[1] + stepped[2] * stepped[2])
            shrink = 1.0 / jnp.maximum(1.0, length / smooth_weight)
            projected = [component * shrink for component in stepped]
            renewed.append(projected)
            divergences.append(backward(projected[0], 0) + backward(projected[1], 1) + backward(projected[2], 2))
        dual_field = renewed
        fidelity = (volume[None] - centers[:, None, None, None]) ** 2
        updated = project_simplex(labelling + tau_step * (jnp.stack(divergences) - fidelity))
        smoothed = 2.0 * updated - labelling
        labelling = updated
        sizes_all = lax.optimization_barrier(jnp.sum(labelling, axis=(1, 2, 3)))
        weighted = lax.optimization_barrier(jnp.sum(labelling * volume[None], axis=(1, 2, 3)))
        centers = (weighted + prior_weight * base_levels) / (sizes_all + prior_weight)
    return (labelling, centers)
```

```python
import jax
import jax.numpy as jnp
from jax import lax
from jax.sharding import PartitionSpec as P

ITERS = 2


tau_step = 0.25
sigma_step = 0.25
smooth_weight = 0.5
prior_weight = 1.0


def with_halo(block, sides, width):
    for axis, dim in sides:
        count = lax.axis_size(axis)
        forward = [(i, i + 1) for i in range(count - 1)]
        backward = [(target, source) for source, target in forward]
        low = lax.ppermute(
            lax.slice_in_dim(block, block.shape[dim] - width, None, axis=dim), axis, forward
        )
        high = lax.ppermute(lax.slice_in_dim(block, 0, width, axis=dim), axis, backward)
        block = jnp.concatenate([low, block, high], axis=dim)
    return block


def project_simplex(values):
    how_many = values.shape[0]
    threshold = None
    for subset in range(1, 1 << how_many):
        members = [label_index for label_index in range(how_many) if subset >> label_index & 1]
        summed = values[members[0]]
        for label_index in members[1:]:
            summed = summed + values[label_index]
        candidate = (summed - 1.0) / float(len(members))
        threshold = candidate if threshold is None else jnp.maximum(threshold, candidate)
    return jnp.maximum(values - threshold[None], 0.0)


def sum_over_devices(partial):
    axes = ("gx", "gy", "gz")
    devices = lax.axis_size(axes)
    flat = jnp.pad(partial.reshape(1, 1, -1), ((0, 0), (0, 0), (0, 128 - partial.size)))
    spread = jnp.broadcast_to(flat, (devices, 1, 128))
    total = lax.all_to_all(spread, axes, 0, 0, tiled=True).sum((0, 1))
    return total[: partial.size].reshape(partial.shape)


def bounds(start, total, extent):
    position = start - 1 + jnp.arange(extent + 1, dtype=jnp.int32)
    return (position >= 0, position < total - 1)


def local(volume, levels):
    thickness = volume.shape[0]
    x_start = (lax.axis_index("gx") * lax.axis_size("gy") + lax.axis_index("gy")) * thickness
    x_total = thickness * lax.axis_size("gx") * lax.axis_size("gy")
    y_start = 0
    y_total = volume.shape[1]
    z_start = lax.axis_index("gz") * volume.shape[2]
    z_total = volume.shape[2] * lax.axis_size("gz")
    extent = volume.shape
    how_many = levels.shape[0]
    inside_x, ahead_x = bounds(x_start, x_total, extent[0])
    inside_y, ahead_y = bounds(y_start, y_total, extent[1])
    inside_z, ahead_z = bounds(z_start, z_total, extent[2])
    inside = (inside_x[:, None, None] & inside_y[None, :, None] & inside_z[None, None, :]).astype(
        jnp.float32
    )
    base_levels = levels.astype(jnp.float32) / 255.0
    centers = base_levels
    starting = (volume[None] - base_levels[:, None, None, None]) ** 2
    labelling = project_simplex(1.0 / how_many - tau_step * starting)
    smoothed = labelling
    dual_field = jnp.zeros((how_many, 3, extent[0] + 1, extent[1] + 1, extent[2] + 1), jnp.float32)
    for iteration in range(ITERS):
        padded = with_halo(smoothed, ((("gx", "gy"), 1), ("gz", 3)), 1)
        padded = jnp.pad(padded, ((0, 0), (0, 0), (1, 1), (0, 0)))
        corner = padded[:, :-1, :-1, :-1]
        grad_x = jnp.where(ahead_x[:, None, None], padded[:, 1:, :-1, :-1] - corner, 0.0)
        grad_y = jnp.where(ahead_y[None, :, None], padded[:, :-1, 1:, :-1] - corner, 0.0)
        grad_z = jnp.where(ahead_z[None, None, :], padded[:, :-1, :-1, 1:] - corner, 0.0)
        stepped = dual_field + sigma_step * jnp.stack([grad_x, grad_y, grad_z], axis=1)
        length = jnp.sqrt(
            stepped[:, 0] * stepped[:, 0]
            + stepped[:, 1] * stepped[:, 1]
            + stepped[:, 2] * stepped[:, 2]
        )
        shrink = inside / jnp.maximum(1.0, length / smooth_weight)
        dual_field = stepped * shrink[:, None]
        divergence = (
            dual_field[:, 0, 1:, 1:, 1:]
            - dual_field[:, 0, :-1, 1:, 1:]
            + (dual_field[:, 1, 1:, 1:, 1:] - dual_field[:, 1, 1:, :-1, 1:])
            + (dual_field[:, 2, 1:, 1:, 1:] - dual_field[:, 2, 1:, 1:, :-1])
        )
        fidelity = (volume[None] - centers[:, None, None, None]) ** 2
        updated = project_simplex(labelling + tau_step * (divergence - fidelity))
        smoothed = 2.0 * updated - labelling
        labelling = updated
        sizes_local = jnp.sum(labelling, axis=(1, 2, 3))
        weighted = jnp.sum(labelling * volume[None], axis=(1, 2, 3))
        sizes_all, weighted_all = sum_over_devices(jnp.stack([sizes_local, weighted]))
        centers = (weighted_all + prior_weight * base_levels) / (sizes_all + prior_weight)
    labelling = lax.all_to_all(labelling, "gy", split_axis=2, concat_axis=1, tiled=True)
    return (labelling, centers)


def solution(mesh):
    return jax.shard_map(
        local,
        mesh=mesh,
        in_specs=(P(("gx", "gy"), None, "gz"), P()),
        out_specs=(P(None, "gx", "gy", "gz"), P()),
        check_vma=False,
    )
```

```python
import functools

import jax
import jax.numpy as jnp
from jax import lax
from jax.experimental import pallas as pl
from jax.experimental.pallas import tpu as pltpu
from jax.sharding import PartitionSpec as P

tau_step = 0.25
sigma_step = 0.25
smooth_weight = 0.5
prior_weight = 1.0

AXES = ("gx", "gy", "gz")
SLABS = ("gx", "gy")
ROWS = 5


def project_simplex(values):
    a, b, c, d = values
    a, b = jnp.maximum(a, b), jnp.minimum(a, b)
    c, d = jnp.maximum(c, d), jnp.minimum(c, d)
    a, c = jnp.maximum(a, c), jnp.minimum(a, c)
    b, d = jnp.maximum(b, d), jnp.minimum(b, d)
    b, c = jnp.maximum(b, c), jnp.minimum(b, c)
    one = a - 1.0
    two = one + b
    three = two + c
    four = three + d
    threshold = jnp.maximum(
        jnp.maximum(one, two * 0.5), jnp.maximum(three * (1.0 / 3.0), four * 0.25)
    )
    return [jnp.maximum(value - threshold, 0.0) for value in values]


def fidelities(volume, centers):
    result = []
    for center in centers:
        apart = volume - center
        result.append(tau_step * (apart * apart))
    return result


def first_labels(volume, base):
    return project_simplex([1.0 / len(base) - value for value in fidelities(volume, base)])


def clip_dual(x, y, z):
    square = x * x + y * y + z * z
    shrink = smooth_weight * lax.rsqrt(jnp.maximum(square, smooth_weight * smooth_weight))
    return x * shrink, y * shrink, z * shrink


class Slab:
    def __init__(self, shape):
        self.shape = shape
        self.y = lax.broadcasted_iota(jnp.int32, shape, 0)
        self.z = lax.broadcasted_iota(jnp.int32, shape, 1)

    def ahead(self, value):
        rows, lanes = self.shape
        y = jnp.where(self.y == rows - 1, 0.0, pltpu.roll(value, rows - 1, 0) - value)
        z = jnp.where(self.z == lanes - 1, 0.0, pltpu.roll(value, lanes - 1, 1) - value)
        return y, z

    def behind(self, y, z):
        before_y = jnp.where(self.y == 0, 0.0, pltpu.roll(y, 1, 0))
        before_z = jnp.where(self.z == 0, 0.0, pltpu.roll(z, 1, 1))
        return (y - before_y) + (z - before_z)


class Planes:
    def __init__(self, shape, height, x_first, x_total):
        self.height = height
        self.lanes = shape[1]
        lane = lax.broadcasted_iota(jnp.int32, shape, 1)
        self.low = lane < height
        self.y = jnp.where(self.low, lane, lane - height)
        self.x = x_first + jnp.where(self.low, 0, 1)
        self.last_x = self.x == x_total - 1
        self.first_x = self.x == 0
        self.inside = (self.x >= 0).astype(jnp.float32)
        self.rows = shape[0]

    def ahead_xy(self, value):
        swapped = pltpu.roll(value, self.height, 1)
        following = jnp.where(self.low, swapped, pltpu.roll(swapped, self.rows - 1, 0))
        x = jnp.where(self.last_x, 0.0, following - value)
        y = jnp.where(
            self.y == self.height - 1, 0.0, pltpu.roll(value, self.lanes - 1, 1) - value
        )
        return x, y

    def behind_xy(self, x, y):
        swapped = pltpu.roll(x, self.height, 1)
        before_x = jnp.where(self.low, pltpu.roll(swapped, 1, 0), swapped)
        before_x = jnp.where(self.first_x, 0.0, before_x)
        before_y = jnp.where(self.y == 0, 0.0, pltpu.roll(y, 1, 1))
        return (x - before_x) + (y - before_y)

    def dual(self, value, next_z, old=None):
        x, y = self.ahead_xy(value)
        z = next_z - value
        x, y, z = (sigma_step * component for component in (x, y, z))
        if old is not None:
            x, y, z = (was + component for was, component in zip(old, (x, y, z)))
        return clip_dual(x, y, z)


def total_of(value):
    return jnp.sum(jnp.sum(value, axis=0, keepdims=True), axis=1, keepdims=True)


def rows_of_base(base_ref):
    return [base_ref[label : label + 1, :] for label in range(base_ref.shape[0])]


def pack_sums(sums, shape):
    lane = lax.broadcasted_iota(jnp.int32, shape, 1)
    row = jnp.zeros(shape, jnp.float32)
    for index, value in enumerate(sums):
        row = jnp.where(lane == index, value, row)
    return row


def slab_index():
    return lax.axis_index("gx") * lax.axis_size("gy") + lax.axis_index("gy")


def neighbours(pair_ref, other_ref, layer, low):
    odd = lax.rem(slab_index(), 2) == 1
    if low:
        return jnp.where(odd, pair_ref[layer], other_ref[layer])
    return jnp.where(odd, other_ref[layer], pair_ref[layer])


def first_kernel(v_ref, pair_ref, other_ref, base_ref, out_ref, lab_ref, dual_ref):
    slabs = lax.axis_size(SLABS)
    blocks = lax.axis_size("gz")
    slab, block = slab_index(), lax.axis_index("gz")
    thick, height, depth = v_ref.shape
    labels = base_ref.shape[0]
    base = rows_of_base(base_ref)
    grid = Slab((height, depth))

    volume = [neighbours(pair_ref, other_ref, thick - 1, True)]
    volume += [v_ref[layer] for layer in range(thick)]
    volume += [neighbours(pair_ref, other_ref, 0, False)]
    for layer, values in enumerate(volume):
        for label, value in enumerate(first_labels(values, base)):
            lab_ref[label, layer] = value
    inside = (slab > 0).astype(jnp.float32)
    open_end = sigma_step * (slab < slabs - 1).astype(jnp.float32)
    for label in range(labels):
        for layer in range(thick + 1):
            value = lab_ref[label, layer]
            x = lab_ref[label, layer + 1] - value
            x = x * (open_end if layer == thick else sigma_step)
            y, z = grid.ahead(value)
            x, y, z = clip_dual(x, sigma_step * y, sigma_step * z)
            if layer == 0:
                dual_ref[label, 0, 0] = x * inside
            else:
                dual_ref[label, 0, layer] = x
                dual_ref[label, 1, layer] = grid.behind(y, z)
    first = jnp.where(block > 0, 0, -1)
    last = jnp.where(block < blocks - 1, depth - 1, depth)
    keep = (grid.z != first) & (grid.z != last)
    sums = [None] * (2 * labels)
    for layer in range(thick):
        values = volume[layer + 1]
        away = fidelities(values, base)
        entries = []
        for label in range(labels):
            divergence = (
                dual_ref[label, 0, layer + 1]
                - dual_ref[label, 0, layer]
                + dual_ref[label, 1, layer + 1]
            )
            entries.append(lab_ref[label, layer + 1] + tau_step * divergence - away[label])
        for label, value in enumerate(project_simplex(entries)):
            value = jnp.where(keep, value, 0.0)
            for index, term in ((label, value), (labels + label, value * values)):
                sums[index] = term if sums[index] is None else sums[index] + term
    devices = slabs * blocks
    turned = jnp.transpose(v_ref[...].reshape(thick * height, depth))
    for row, plane in enumerate((0, 1, depth - 2, depth - 1)):
        out_ref[pl.ds(row, devices, stride=ROWS), :] = jnp.broadcast_to(
            turned[plane : plane + 1], (devices, thick * height)
        )
    packed = pack_sums([total_of(value) for value in sums], (1, thick * height))
    out_ref[pl.ds(ROWS - 1, devices, stride=ROWS), :] = jnp.broadcast_to(
        packed, (devices, thick * height)
    )


def ahead_kernel(
    v_ref, pair_ref, other_ref, base_ref, w_ref, q_ref, lab_ref, dual_ref, smooth_ref
):
    slabs = lax.axis_size(SLABS)
    slab = slab_index()
    thick, height, depth = v_ref.shape
    labels = base_ref.shape[0]
    base = rows_of_base(base_ref)
    grid = Slab((height, depth))
    halo = thick
    layers = thick + 2 * halo

    def layer_of(index):
        if index < halo:
            return neighbours(pair_ref, other_ref, index, True)
        if index < halo + thick:
            return v_ref[index - halo]
        return neighbours(pair_ref, other_ref, index - halo - thick, False)

    for layer in range(layers):
        for label, value in enumerate(first_labels(layer_of(layer), base)):
            lab_ref[label, layer] = value
    inside = (slab > 0).astype(jnp.float32)
    open_end = sigma_step * (slab < slabs - 1).astype(jnp.float32)
    end = halo + thick - 1
    for label in range(labels):
        for layer in range(layers - 1):
            value = lab_ref[label, layer]
            x = lab_ref[label, layer + 1] - value
            x = x * (open_end if layer == end else sigma_step)
            y, z = grid.ahead(value)
            x, y, z = clip_dual(x, sigma_step * y, sigma_step * z)
            dual_ref[label, 0, layer] = x * inside if layer == halo - 1 else x
            dual_ref[label, 1, layer] = y
            dual_ref[label, 2, layer] = z
    for layer in range(1, layers - 1):
        away = fidelities(layer_of(layer), base)
        entries = []
        for label in range(labels):
            divergence = (
                dual_ref[label, 0, layer]
                - dual_ref[label, 0, layer - 1]
                + grid.behind(dual_ref[label, 1, layer], dual_ref[label, 2, layer])
            )
            entries.append(lab_ref[label, layer] + tau_step * divergence - away[label])
        for label, value in enumerate(project_simplex(entries)):
            smooth_ref[label, layer] = 2.0 * value - lab_ref[label, layer]
            lab_ref[label, layer] = value
    for label in range(labels):
        before = None
        for layer in range(halo - 1, halo + thick):
            value = smooth_ref[label, layer]
            x = smooth_ref[label, layer + 1] - value
            x = x * (open_end if layer == end else sigma_step)
            y, z = grid.ahead(value)
            x, y, z = clip_dual(
                dual_ref[label, 0, layer] + x,
                dual_ref[label, 1, layer] + sigma_step * y,
                dual_ref[label, 2, layer] + sigma_step * z,
            )
            if layer == halo - 1:
                x = x * inside
            else:
                divergence = (x - before) + grid.behind(y, z)
                w_ref[label, layer - halo] = lab_ref[label, layer] + tau_step * divergence
            before = x
    row = lax.broadcasted_iota(jnp.int32, (8, thick * height), 0)
    near, far = [], []
    for start in (0, halo, halo + thick):
        flat = jnp.concatenate([layer_of(start + index) for index in range(thick)], axis=0)
        turned = jnp.transpose(flat)
        near.append(turned[0:8])
        far.append(turned[depth - 8 : depth])
    for column in range(6):
        plane = jnp.zeros((8, thick * height), jnp.float32)
        for which in range(3):
            if column >= 2:
                source = near[which][column - 2 : column - 1]
                plane = jnp.where(row == which, source, plane)
            if column < 4:
                source = far[which][4 + column : 5 + column]
                plane = jnp.where(row == 4 + which, source, plane)
        q_ref[column] = plane


def last_kernel(
    v_ref, w_ref, q_ref, base_ref, got_ref, sums_ref, *rest
):
    slabs = lax.axis_size(SLABS)
    blocks = lax.axis_size("gz")
    count = lax.axis_size("gy")
    slab, block = slab_index(), lax.axis_index("gz")
    pieces, lab_ref = rest[:count], rest[count]
    thick, height, depth = v_ref.shape
    lanes = thick * height
    labels = base_ref.shape[0]
    base = rows_of_base(base_ref)
    devices = slabs * blocks
    x_total = slabs * thick

    row = lax.broadcasted_iota(jnp.int32, (slabs, lanes), 0)
    everywhere = Planes((slabs, lanes), height, thick * row, x_total)
    sums = [jnp.zeros((slabs, lanes), jnp.float32) for _ in range(2 * labels)]
    for end in range(blocks - 1):
        planes = [
            got_ref[pl.ds((end + beyond) * ROWS + which, slabs, stride=blocks * ROWS), :]
            for beyond, which in ((0, 2), (0, 3), (1, 0), (1, 1))
        ]
        first = [first_labels(plane, base) for plane in planes]
        divergence = [[], []]
        for label in range(labels):
            duals = [
                everywhere.dual(first[index][label], first[index + 1][label])
                for index in range(3)
            ]
            for index in (1, 2):
                x, y, z = duals[index]
                divergence[index - 1].append(
                    everywhere.behind_xy(x, y) + (z - duals[index - 1][2])
                )
        for index in (1, 2):
            away = fidelities(planes[index], base)
            entries = [
                first[index][label] + tau_step * divergence[index - 1][label] - away[label]
                for label in range(labels)
            ]
            for label, value in enumerate(project_simplex(entries)):
                sums[label] = sums[label] + value
                sums[labels + label] = sums[labels + label] + value * planes[index]
    parts = got_ref[pl.ds(ROWS - 1, devices, stride=ROWS), :]
    lane = lax.broadcasted_iota(jnp.int32, (1, lanes), 1)
    parts = jnp.sum(parts, axis=0, keepdims=True)
    for index, value in enumerate(sums):
        parts = parts + jnp.where(lane == index, total_of(value), 0.0)
    whole = [
        jnp.sum(jnp.where(lane == index, parts, 0.0), axis=1, keepdims=True)
        for index in range(2 * labels)
    ]
    centers = [
        (whole[labels + label] + prior_weight * base[label]) / (whole[label] + prior_weight)
        for label in range(labels)
    ]

    row = lax.broadcasted_iota(jnp.int32, (8, lanes), 0)
    local = Planes((8, lanes), height, thick * (slab - 1 + (row & 3)), x_total)
    planes = [q_ref[column] for column in range(6)]
    for which in range(3):
        index = jnp.clip(slab - 1 + which, 0, slabs - 1) * blocks
        low = (index + jnp.maximum(block - 1, 0)) * ROWS
        high = (index + jnp.minimum(block + 1, blocks - 1)) * ROWS
        for column in range(2):
            source = got_ref[pl.ds(low + 2 + column, 1), :]
            planes[column] = jnp.where(row == which, source, planes[column])
            source = got_ref[pl.ds(high + column, 1), :]
            planes[4 + column] = jnp.where(row == 4 + which, source, planes[4 + column])
    first = [first_labels(plane, base) for plane in planes]
    duals = []
    for label in range(labels):
        duals.append([])
        for column in range(5):
            x, y, z = local.dual(first[column][label], first[column + 1][label])
            duals[label].append((x * local.inside, y, z))
    second, smooth = {}, {}
    for column in range(1, 5):
        away = fidelities(planes[column], base)
        entries = []
        for label in range(labels):
            x, y, z = duals[label][column]
            divergence = local.behind_xy(x, y) + (z - duals[label][column - 1][2])
            entries.append(first[column][label] + tau_step * divergence - away[label])
        second[column] = project_simplex(entries)
        smooth[column] = [
            2.0 * second[column][label] - first[column][label] for label in range(labels)
        ]
    for label in range(labels):
        for column in range(1, 4):
            x, y, z = local.dual(
                smooth[column][label], smooth[column + 1][label], duals[label][column]
            )
            duals[label][column] = (x * local.inside, y, z)
    edge = {}
    for column in (2, 3):
        away = fidelities(planes[column], centers)
        entries = []
        for label in range(labels):
            x, y, z = duals[label][column]
            divergence = local.behind_xy(x, y) + (z - duals[label][column - 1][2])
            entries.append(second[column][label] + tau_step * divergence - away[label])
        edge[column] = project_simplex(entries)
    step = depth // labels
    tiles = [jnp.zeros((8, lanes), jnp.float32) for _ in range(depth // 8)]
    for label in range(labels):
        two, three = edge[2][label], edge[3][label]
        tiles[label * step // 8] = tiles[label * step // 8] + jnp.where(
            row == 0, pltpu.roll(two, 7, 0), jnp.where(row == 1, three, 0.0)
        )
        place = (label * step // 8 - 1) % (depth // 8)
        tiles[place] = tiles[place] + jnp.where(
            row == 6, pltpu.roll(two, 1, 0), jnp.where(row == 7, pltpu.roll(three, 2, 0), 0.0)
        )
    columns = jnp.transpose(jnp.concatenate(tiles, axis=0))

    z = lax.broadcasted_iota(jnp.int32, (height, depth), 1)
    replaced = ((z < 2) & (block > 0)) | ((z >= depth - 2) & (block < blocks - 1))
    sums = [None] * (2 * labels)
    for layer in range(thick):
        values = v_ref[layer]
        away = fidelities(values, centers)
        entries = [w_ref[label, layer] - away[label] for label in range(labels)]
        for label, value in enumerate(project_simplex(entries)):
            column = columns[layer * height : (layer + 1) * height]
            if label:
                column = pltpu.roll(column, depth - label * step, 1)
            value = jnp.where(replaced, column, value)
            lab_ref[label, layer] = value
            for index, term in ((label, value), (labels + label, value * values)):
                sums[index] = term if sums[index] is None else sums[index] + term
    packed = pack_sums([total_of(value) for value in sums], (1, lanes))
    sums_ref[...] = jnp.broadcast_to(packed, (devices, lanes))
    rows = height // count
    me = lax.axis_index("gy")
    for other in range(count):
        start = pl.multiple_of((me ^ other) * rows, rows)
        pieces[other][...] = lab_ref[:, :, pl.ds(start, rows), :]


def join_kernel(*refs):
    *pieces, out_ref = refs
    me = lax.axis_index("gy")
    thick = pieces[0].shape[1]
    for other, piece in enumerate(pieces):
        out_ref[:, pl.ds((me ^ other) * thick, thick)] = piece[...]


def local(volume, levels):
    slabs = lax.axis_size(SLABS)
    blocks = lax.axis_size("gz")
    count = lax.axis_size("gy")
    devices = slabs * blocks
    thick, height, depth = volume.shape
    labels = levels.shape[0]
    lanes = thick * height
    if thick != 2 or labels != 4 or count & (count - 1):
        raise ValueError("unsupported sizes")
    f32 = functools.partial(jax.ShapeDtypeStruct, dtype=jnp.float32)
    vmem = pl.BlockSpec(memory_space=pltpu.VMEM)

    base_levels = levels.astype(jnp.float32) / 255.0
    base = jnp.broadcast_to(base_levels[:, None], (labels, lanes))

    pairs = [(i, i ^ 1) for i in range(slabs)]
    across = [(i, i + 1) for i in range(1, slabs - 1, 2)]
    across += [(target, source) for source, target in across]
    other = lax.ppermute(volume, SLABS, across)
    pair = lax.ppermute(volume, SLABS, pairs)

    sent = pl.pallas_call(
        first_kernel,
        out_shape=f32((devices * ROWS, lanes)),
        in_specs=[vmem] * 4,
        out_specs=vmem,
        scratch_shapes=[
            pltpu.VMEM((labels, thick + 2, height, depth), jnp.float32),
            pltpu.VMEM((labels, 2, thick + 1, height, depth), jnp.float32),
        ],
        name="first",
    )(volume, pair, other, base)
    got = lax.all_to_all(sent.reshape(devices, 1, ROWS * lanes), AXES, 0, 0, tiled=True)
    got = got.reshape(devices * ROWS, lanes)

    layers = 3 * thick
    ahead, planes = pl.pallas_call(
        ahead_kernel,
        out_shape=[f32((labels, thick, height, depth)), f32((6, 8, lanes))],
        in_specs=[vmem] * 4,
        out_specs=[vmem] * 2,
        scratch_shapes=[
            pltpu.VMEM((labels, layers, height, depth), jnp.float32),
            pltpu.VMEM((labels, 3, layers, height, depth), jnp.float32),
            pltpu.VMEM((labels, layers, height, depth), jnp.float32),
        ],
        cost_estimate=pl.CostEstimate(
            flops=200 * labels * layers * height * depth,
            bytes_accessed=4 * 20 * height * depth,
            transcendentals=0,
        ),
        name="ahead",
    )(volume, pair, other, base)

    piece = f32((labels, thick, height // count, depth))
    sums, *pieces = pl.pallas_call(
        last_kernel,
        out_shape=[f32((devices, lanes))] + [piece] * count,
        in_specs=[vmem] * 5,
        out_specs=[vmem] * (count + 1),
        scratch_shapes=[pltpu.VMEM((labels, thick, height, depth), jnp.float32)],
        name="last",
    )(volume, ahead, planes, base, got)

    total = lax.all_to_all(sums.reshape(devices, 1, lanes), AXES, 0, 0, tiled=True)
    for shift in range(1, count):
        pieces[shift] = lax.ppermute(
            pieces[shift], "gy", [(i, i ^ shift) for i in range(count)]
        )
    labelling = pl.pallas_call(
        join_kernel,
        out_shape=f32((labels, thick * count, height // count, depth)),
        in_specs=[vmem] * count,
        out_specs=vmem,
        cost_estimate=pl.CostEstimate(
            flops=labels * thick * height * depth,
            bytes_accessed=8 * labels * thick * height * depth,
            transcendentals=0,
        ),
        name="join",
    )(*pieces)
    total = total.sum((0, 1))
    sizes_all, weighted_all = total[:labels], total[labels : 2 * labels]
    centers = (weighted_all + prior_weight * base_levels) / (sizes_all + prior_weight)
    return (labelling, centers)


def solution(mesh):
    return jax.shard_map(
        local,
        mesh=mesh,
        in_specs=(P(("gx", "gy"), None, "gz"), P()),
        out_specs=(P(None, "gx", "gy", "gz"), P()),
        check_vma=False,
    )
```

```python
import functools

import jax
import jax.numpy as jnp
from jax import lax
from jax.experimental import pallas as pl
from jax.experimental.pallas import tpu as pltpu
from jax.sharding import PartitionSpec as P


tau_step = 0.25
prior_weight = 1.0


AXES = ("gx", "gy", "gz")
SLABS = ("gx", "gy")
ROWS = 5


def project_simplex(values, total):
    a, b, c, d = values
    a, b = jnp.maximum(a, b), jnp.minimum(a, b)
    c, d = jnp.maximum(c, d), jnp.minimum(c, d)
    a, c = jnp.maximum(a, c), jnp.minimum(a, c)
    b, d = jnp.maximum(b, d), jnp.minimum(b, d)
    b, c = jnp.maximum(b, c), jnp.minimum(b, c)
    one = a - total
    two = one + b
    three = two + c
    four = three + d
    threshold = jnp.maximum(
        jnp.maximum(one, two * 0.5), jnp.maximum(three * (1.0 / 3.0), four * 0.25)
    )
    return [jnp.maximum(value - threshold, 0.0) for value in values]


def affine(centers, unit):
    return [
        (center * (2.0 * unit * tau_step), center * center * (unit * tau_step))
        for center in centers
    ]


def attraction(volume, terms):
    return [volume * slope - offset for slope, offset in terms]


def shrink_of(x, y, z):
    return lax.rsqrt(jnp.maximum(x * x + y * y + z * z, 1.0))


class Planes:
    def __init__(self, shape, height, x_first, x_total):
        self.height = height
        self.rows, self.lanes = shape
        lane = lax.broadcasted_iota(jnp.int32, shape, 1)
        self.low = lane < height
        y = jnp.where(self.low, lane, lane - height)
        x = x_first + jnp.where(self.low, 0, 1)
        self.open_x = (x != x_total - 1).astype(jnp.float32)
        self.open_y = (y != height - 1).astype(jnp.float32)
        self.inside = (x >= 0).astype(jnp.float32)

    def dual(self, value, next_z, old=None):
        swapped = pltpu.roll(value, self.height, 1)
        following = jnp.where(self.low, swapped, pltpu.roll(swapped, self.rows - 1, 0))
        x = (following - value) * self.open_x
        y = (pltpu.roll(value, self.lanes - 1, 1) - value) * self.open_y
        z = next_z - value
        if old is not None:
            x, y, z = old[0] + x, old[1] + y, old[2] + z
        shrink = shrink_of(x, y, z)
        return x * shrink, y * shrink, z * shrink

    def behind_xy(self, x, y):
        swapped = pltpu.roll(x, self.height, 1)
        before_x = jnp.where(self.low, pltpu.roll(swapped, 1, 0), swapped)
        return (x - before_x) + (y - pltpu.roll(y, 1, 1))


def total_of(value):
    return jnp.sum(jnp.sum(value, axis=0, keepdims=True), axis=1, keepdims=True)


def base_kernel(levels_ref, base_ref):
    values = levels_ref[...].astype(jnp.float32) / 255.0
    for label in range(values.shape[1]):
        base_ref[label : label + 1] = jnp.broadcast_to(
            values[:, label : label + 1], (1, base_ref.shape[1])
        )


def base_of(base_ref):
    return [base_ref[label : label + 1] for label in range(base_ref.shape[0])]


def pack_sums(sums, shape):
    lane = lax.broadcasted_iota(jnp.int32, shape, 1)
    row = jnp.zeros(shape, jnp.float32)
    for index, value in enumerate(sums):
        row = jnp.where(lane == index, total_of(value), row)
    return row


def slab_index():
    return lax.axis_index("gx") * lax.axis_size("gy") + lax.axis_index("gy")


def open_lanes(depth):
    lane = lax.broadcasted_iota(jnp.int32, (1, depth), 1)
    return (lane != depth - 1).astype(jnp.float32)


def volume_layers(v_ref, pair_ref, other_ref, halo):
    thick = v_ref.shape[0]
    odd = lax.rem(slab_index(), 2) == 1

    def read(layer, rows=slice(None)):
        if layer < halo:
            layer += thick - halo
            return jnp.where(odd, pair_ref[layer, rows], other_ref[layer, rows])
        layer -= halo
        if layer < thick:
            return v_ref[layer, rows]
        layer -= thick
        return jnp.where(odd, other_ref[layer, rows], pair_ref[layer, rows])

    return read


def add_to(sums, index, term):
    sums[index] = term if sums[index] is None else sums[index] + term


CHUNK = 16
BASE_FLOPS = 50_000_000


def store_padded(ref, where, start, value, height):
    rows = value.shape[0]
    ref[where + (slice(start, start + rows),)] = value
    if start + rows == height:
        ref[where + (slice(height, height + 1),)] = value[rows - 1 :]


def first_halves(read, layers, height, terms, h_ref):
    for layer in layers:
        for start in range(0, height, CHUNK):
            values = read(layer, slice(start, start + CHUNK))
            for label, half in enumerate(project_simplex(attraction(values, terms), 0.5)):
                store_padded(h_ref, (label, layer), start, half, height)


def gradient(h_ref, label, layer, height, depth, open_z):
    half = h_ref[label, layer, 0:height]
    x = h_ref[label, layer + 1, 0:height] - half
    y = h_ref[label, layer, 1 : height + 1] - half
    z = (pltpu.roll(half, depth - 1, 1) - half) * open_z
    return x, y, z


def behind_yz(y, z, y_ref, where, height):
    y_ref[where + (slice(0, 8),)] = jnp.zeros((8, y.shape[1]), jnp.float32)
    y_ref[where + (slice(8, 8 + height),)] = y
    return (y - y_ref[where + (slice(7, 7 + height),)]) + (z - pltpu.roll(z, 1, 1))


def first_kernel(
    v_hbm, pair_ref, other_ref, base_ref, out_ref, v_ref, h_ref, y_ref, divergence_ref, arrived
):
    copy = pltpu.make_async_copy(v_hbm, v_ref, arrived)
    copy.start()
    slabs = lax.axis_size(SLABS)
    blocks = lax.axis_size("gz")
    slab, block = slab_index(), lax.axis_index("gz")
    thick, height, depth = v_hbm.shape
    lanes = thick * height
    devices = slabs * blocks
    labels = base_ref.shape[0]
    terms = affine(base_of(base_ref), 0.5)
    open_z = open_lanes(depth)
    read = volume_layers(v_ref, pair_ref, other_ref, 1)

    first_halves(read, (0, thick + 1), height, terms, h_ref)
    copy.wait()
    first_halves(read, range(1, thick + 1), height, terms, h_ref)
    turned = jnp.transpose(v_ref[...].reshape(lanes, depth))
    for row, plane in enumerate((0, 1, depth - 2, depth - 1)):
        out_ref[pl.ds(row, devices, stride=ROWS), :] = jnp.broadcast_to(
            turned[plane : plane + 1], (devices, lanes)
        )
    inside = (slab > 0).astype(jnp.float32)
    open_x = (slab < slabs - 1).astype(jnp.float32)
    for label in range(labels):
        before = None
        for layer in range(thick + 1):
            x, y, z = gradient(h_ref, label, layer, height, depth, open_z)
            if layer == thick:
                x = x * open_x
            shrink = shrink_of(x, y, z)
            x = x * shrink
            if layer == 0:
                x = x * inside
            else:
                where = (label, layer - 1)
                divergence_ref[where] = (x - before) + behind_yz(
                    y * shrink, z * shrink, y_ref, where, height
                )
            before = x
    sums = [None] * (2 * labels)
    for layer in range(thick):
        for start in range(0, height, CHUNK):
            rows = slice(start, start + CHUNK)
            values = v_ref[layer, rows]
            entries = [
                h_ref[label, layer + 1, rows] + 0.0625 * divergence_ref[label, layer, rows] + term
                for label, term in enumerate(attraction(values, terms))
            ]
            for label, value in enumerate(project_simplex(entries, 0.5)):
                add_to(sums, label, value)
                add_to(sums, labels + label, value * values)
    lane = lax.broadcasted_iota(jnp.int32, (CHUNK, depth), 1)
    first = jnp.where(block > 0, 0, -1)
    last = jnp.where(block < blocks - 1, depth - 1, depth)
    keep = (lane != first) & (lane != last)
    sums = [jnp.where(keep, value, 0.0) for value in sums]
    out_ref[pl.ds(ROWS - 1, devices, stride=ROWS), :] = jnp.broadcast_to(
        pack_sums(sums, (1, lanes)), (devices, lanes)
    )


def ahead_kernel(
    v_ref, pair_ref, other_ref, base_ref, w_ref, q_ref, h_ref, s_ref, dual_ref, y_ref, l_ref
):
    slabs = lax.axis_size(SLABS)
    slab = slab_index()
    thick, height, depth = v_ref.shape
    lanes = thick * height
    labels = base_ref.shape[0]
    terms = affine(base_of(base_ref), 0.5)
    open_z = open_lanes(depth)
    halo = thick
    layers = thick + 2 * halo
    read = volume_layers(v_ref, pair_ref, other_ref, halo)

    first_halves(read, range(layers), height, terms, h_ref)
    inside = (slab > 0).astype(jnp.float32)
    open_x = (slab < slabs - 1).astype(jnp.float32)
    end = halo + thick - 1
    for label in range(labels):
        before = None
        for layer in range(layers - 1):
            x, y, z = gradient(h_ref, label, layer, height, depth, open_z)
            if layer == end:
                x = x * open_x
            shrink = shrink_of(x, y, z)
            x = x * shrink
            if layer == halo - 1:
                x = x * inside
            if layer:
                y, z = y * shrink, z * shrink
                where = (label, layer)
                dual_ref[label, 0, layer] = x
                dual_ref[label, 1, layer] = y
                dual_ref[label, 2, layer] = z
                l_ref[where] = (x - before) + behind_yz(y, z, y_ref, where, height)
            before = x
    for layer in range(1, layers - 1):
        for start in range(0, height, CHUNK):
            rows = slice(start, start + CHUNK)
            values = read(layer, rows)
            halves = [h_ref[label, layer, rows] for label in range(labels)]
            entries = [
                halves[label] + 0.0625 * l_ref[label, layer, rows] + term
                for label, term in enumerate(attraction(values, terms))
            ]
            for label, value in enumerate(project_simplex(entries, 0.5)):
                value = value + value
                store_padded(s_ref, (label, layer), start, value - halves[label], height)
                l_ref[label, layer, rows] = value
    for label in range(labels):
        before = None
        for layer in range(halo - 1, halo + thick):
            x, y, z = gradient(s_ref, label, layer, height, depth, open_z)
            if layer == end:
                x = x * open_x
            x = dual_ref[label, 0, layer] + x
            y = dual_ref[label, 1, layer] + y
            z = dual_ref[label, 2, layer] + z
            shrink = shrink_of(x, y, z)
            x = x * shrink
            if layer == halo - 1:
                x = x * inside
            else:
                divergence = (x - before) + behind_yz(
                    y * shrink, z * shrink, y_ref, (label, layer), height
                )
                w_ref[label, layer - halo] = l_ref[label, layer] + 0.125 * divergence
            before = x
    row = lax.broadcasted_iota(jnp.int32, (8, lanes), 0)
    near, far = [], []
    for start in (0, halo, halo + thick):
        turned = jnp.transpose(
            jnp.concatenate([read(start + index) for index in range(thick)], axis=0)
        )
        near.append(turned[0:8])
        far.append(turned[depth - 8 : depth])
    for column in range(6):
        plane = jnp.zeros((8, lanes), jnp.float32)
        for which in range(3):
            if column >= 2:
                plane = jnp.where(row == which, near[which][column - 2 : column - 1], plane)
            if column < 4:
                plane = jnp.where(row == 4 + which, far[which][4 + column : 5 + column], plane)
        q_ref[column] = plane


def last_kernel(v_ref, w_ref, q_ref, base_ref, got_ref, sums_ref, *rest):
    slabs = lax.axis_size(SLABS)
    blocks = lax.axis_size("gz")
    count = lax.axis_size("gy")
    slab, block = slab_index(), lax.axis_index("gz")
    pieces, lab_ref = rest[:count], rest[count]
    thick, height, depth = v_ref.shape
    lanes = thick * height
    labels = base_ref.shape[0]
    base = base_of(base_ref)
    terms = affine(base, 0.5)
    devices = slabs * blocks
    x_total = slabs * thick

    row = lax.broadcasted_iota(jnp.int32, (slabs, lanes), 0)
    everywhere = Planes((slabs, lanes), height, thick * row, x_total)
    sums = [None] * (2 * labels)
    for end in range(blocks - 1):
        planes = [
            got_ref[pl.ds((end + beyond) * ROWS + which, slabs, stride=blocks * ROWS), :]
            for beyond, which in ((0, 2), (0, 3), (1, 0), (1, 1))
        ]
        pulls = [attraction(plane, terms) for plane in planes]
        first = [project_simplex(pull, 0.5) for pull in pulls]
        divergence = [[], []]
        for label in range(labels):
            duals = [
                everywhere.dual(first[index][label], first[index + 1][label])
                for index in range(3)
            ]
            for index in (1, 2):
                x, y, z = duals[index]
                divergence[index - 1].append(
                    everywhere.behind_xy(x, y) + (z - duals[index - 1][2])
                )
        for index in (1, 2):
            entries = [
                first[index][label] + 0.0625 * divergence[index - 1][label] + pulls[index][label]
                for label in range(labels)
            ]
            for label, value in enumerate(project_simplex(entries, 0.5)):
                add_to(sums, label, value)
                add_to(sums, labels + label, value * planes[index])
    parts = got_ref[pl.ds(ROWS - 1, devices, stride=ROWS), :]
    lane = lax.broadcasted_iota(jnp.int32, (1, lanes), 1)
    parts = jnp.sum(parts, axis=0, keepdims=True)
    if blocks > 1:
        parts = parts + pack_sums(sums, (1, lanes))
    whole = [
        2.0 * jnp.sum(jnp.where(lane == index, parts, 0.0), axis=1, keepdims=True)
        for index in range(2 * labels)
    ]
    centers = [
        (whole[labels + label] + prior_weight * base[label]) / (whole[label] + prior_weight)
        for label in range(labels)
    ]

    row = lax.broadcasted_iota(jnp.int32, (8, lanes), 0)
    local = Planes((8, lanes), height, thick * (slab - 1 + (row & 3)), x_total)
    planes = [q_ref[column] for column in range(6)]
    for which in range(3):
        index = jnp.clip(slab - 1 + which, 0, slabs - 1) * blocks
        low = (index + jnp.maximum(block - 1, 0)) * ROWS
        high = (index + jnp.minimum(block + 1, blocks - 1)) * ROWS
        for column in range(2):
            source = got_ref[pl.ds(low + 2 + column, 1), :]
            planes[column] = jnp.where(row == which, source, planes[column])
            source = got_ref[pl.ds(high + column, 1), :]
            planes[4 + column] = jnp.where(row == 4 + which, source, planes[4 + column])
    pulls = [attraction(plane, terms) for plane in planes]
    first = [project_simplex(pull, 0.5) for pull in pulls]
    duals = []
    for label in range(labels):
        duals.append([])
        for column in range(5):
            x, y, z = local.dual(first[column][label], first[column + 1][label])
            duals[label].append((x * local.inside, y, z))
    second, smooth = {}, {}
    for column in range(1, 5):
        entries = []
        for label in range(labels):
            x, y, z = duals[label][column]
            divergence = local.behind_xy(x, y) + (z - duals[label][column - 1][2])
            entries.append(first[column][label] + 0.0625 * divergence + pulls[column][label])
        second[column] = [value + value for value in project_simplex(entries, 0.5)]
        smooth[column] = [
            second[column][label] - first[column][label] for label in range(labels)
        ]
    for label in range(labels):
        for column in range(1, 4):
            x, y, z = local.dual(
                smooth[column][label], smooth[column + 1][label], duals[label][column]
            )
            duals[label][column] = (x * local.inside, y, z)
    terms = affine(centers, 1.0)
    edge = {}
    for column in (2, 3):
        pull = attraction(planes[column], terms)
        entries = []
        for label in range(labels):
            x, y, z = duals[label][column]
            divergence = local.behind_xy(x, y) + (z - duals[label][column - 1][2])
            entries.append(second[column][label] + 0.125 * divergence + pull[label])
        edge[column] = project_simplex(entries, 1.0)
    step = depth // labels
    tiles = [jnp.zeros((8, lanes), jnp.float32) for _ in range(depth // 8)]
    for label in range(labels):
        two, three = edge[2][label], edge[3][label]
        place = label * step // 8
        tiles[place] = tiles[place] + jnp.where(
            row == 0, pltpu.roll(two, 7, 0), jnp.where(row == 1, three, 0.0)
        )
        place = (place - 1) % (depth // 8)
        tiles[place] = tiles[place] + jnp.where(
            row == 6, pltpu.roll(two, 1, 0), jnp.where(row == 7, pltpu.roll(three, 2, 0), 0.0)
        )
    columns = jnp.transpose(jnp.concatenate(tiles, axis=0))

    z = lax.broadcasted_iota(jnp.int32, (CHUNK, depth), 1)
    replaced = ((z < 2) & (block > 0)) | ((z >= depth - 2) & (block < blocks - 1))
    sums = [None] * (2 * labels)
    for layer in range(thick):
        for start in range(0, height, CHUNK):
            rows = slice(start, start + CHUNK)
            values = v_ref[layer, rows]
            entries = [
                w_ref[label, layer, rows] + pull
                for label, pull in enumerate(attraction(values, terms))
            ]
            for label, value in enumerate(project_simplex(entries, 1.0)):
                column = columns[layer * height + start : layer * height + start + CHUNK]
                if label:
                    column = pltpu.roll(column, depth - label * step, 1)
                value = jnp.where(replaced, column, value)
                lab_ref[label, layer, rows] = value
                add_to(sums, label, value)
                add_to(sums, labels + label, value * values)
    sums_ref[...] = jnp.broadcast_to(pack_sums(sums, (1, lanes)), (devices, lanes))
    rows = height // count
    me = lax.axis_index("gy")
    for other in range(count):
        start = pl.multiple_of((me ^ other) * rows, rows)
        pieces[other][...] = lab_ref[:, :, pl.ds(start, rows), :]


def join_kernel(*refs):
    *pieces, out_ref = refs
    me = lax.axis_index("gy")
    thick = pieces[0].shape[1]
    for other, piece in enumerate(pieces):
        out_ref[:, pl.ds((me ^ other) * thick, thick)] = piece[...]


def local(volume, levels):
    slabs = lax.axis_size(SLABS)
    blocks = lax.axis_size("gz")
    count = lax.axis_size("gy")
    devices = slabs * blocks
    thick, height, depth = volume.shape
    labels = levels.shape[0]
    lanes = thick * height
    if thick != 2 or labels != 4 or count & (count - 1):
        raise ValueError("unsupported sizes")
    f32 = functools.partial(jax.ShapeDtypeStruct, dtype=jnp.float32)
    vmem = pl.BlockSpec(memory_space=pltpu.VMEM)

    base_levels = levels.astype(jnp.float32) / 255.0
    params = pltpu.CompilerParams(vmem_limit_bytes=8 << 20)
    base = pl.pallas_call(
        base_kernel,
        out_shape=f32((labels, lanes)),
        in_specs=[vmem],
        out_specs=vmem,
        compiler_params=params,
        cost_estimate=pl.CostEstimate(flops=BASE_FLOPS, bytes_accessed=0, transcendentals=0),
        name="base",
    )(levels.reshape(1, labels))

    pairs = [(i, i ^ 1) for i in range(slabs)]
    across = [(i, i + 1) for i in range(1, slabs - 1, 2)]
    across += [(target, source) for source, target in across]
    pair = lax.ppermute(volume, SLABS, pairs)
    other = lax.ppermute(volume, SLABS, across)

    sent, volume = pl.pallas_call(
        first_kernel,
        out_shape=[f32((devices * ROWS, lanes)), f32(volume.shape)],
        in_specs=[pl.BlockSpec(memory_space=pltpu.HBM)] + [vmem] * 3,
        out_specs=[vmem] * 2,
        scratch_shapes=[
            pltpu.VMEM((labels, thick + 2, height + 8, depth), jnp.float32),
            pltpu.VMEM((labels, thick, height + 8, depth), jnp.float32),
            pltpu.VMEM((labels, thick, height, depth), jnp.float32),
            pltpu.SemaphoreType.DMA,
        ],
        compiler_params=params,
        name="first",
    )(volume, pair, other, base)
    got = lax.all_to_all(sent.reshape(devices, 1, ROWS * lanes), AXES, 0, 0, tiled=True)
    got = got.reshape(devices * ROWS, lanes)

    layers = 3 * thick
    ahead, planes = pl.pallas_call(
        ahead_kernel,
        out_shape=[f32((labels, thick, height, depth)), f32((6, 8, lanes))],
        in_specs=[vmem] * 4,
        out_specs=[vmem] * 2,
        scratch_shapes=[
            pltpu.VMEM((labels, layers, height + 8, depth), jnp.float32),
            pltpu.VMEM((labels, layers, height + 8, depth), jnp.float32),
            pltpu.VMEM((labels, 3, layers, height, depth), jnp.float32),
            pltpu.VMEM((labels, layers, height + 8, depth), jnp.float32),
            pltpu.VMEM((labels, layers, height, depth), jnp.float32),
        ],
        cost_estimate=pl.CostEstimate(
            flops=200 * labels * layers * height * depth,
            bytes_accessed=4 * 20 * height * depth,
            transcendentals=0,
        ),
        compiler_params=params,
        name="ahead",
    )(volume, pair, other, base)

    piece = f32((labels, thick, height // count, depth))
    sums, *pieces = pl.pallas_call(
        last_kernel,
        out_shape=[f32((devices, lanes))] + [piece] * count,
        in_specs=[vmem] * 5,
        out_specs=[vmem] * (count + 1),
        scratch_shapes=[pltpu.VMEM((labels, thick, height, depth), jnp.float32)],
        compiler_params=params,
        name="last",
    )(volume, ahead, planes, base, got)

    total = lax.all_to_all(sums.reshape(devices, 1, lanes), AXES, 0, 0, tiled=True)
    for shift in range(1, count):
        pieces[shift] = lax.ppermute(pieces[shift], "gy", [(i, i ^ shift) for i in range(count)])
    join = pl.pallas_call(
        join_kernel,
        out_shape=f32((labels, thick * count, height // count, depth)),
        in_specs=[vmem] * count,
        out_specs=vmem,
        cost_estimate=pl.CostEstimate(
            flops=labels * thick * height * depth,
            bytes_accessed=8 * labels * thick * height * depth,
            transcendentals=0,
        ),
        compiler_params=params,
        name="join",
    )
    labelling = join(*pieces)
    total = total.sum((0, 1))
    sizes_all, weighted_all = total[:labels], total[labels : 2 * labels]
    centers = (weighted_all + prior_weight * base_levels) / (sizes_all + prior_weight)
    return (labelling, centers)


def solution(mesh):
    return jax.shard_map(
        local,
        mesh=mesh,
        in_specs=(P(("gx", "gy"), None, "gz"), P()),
        out_specs=(P(None, "gx", "gy", "gz"), P()),
        check_vma=False,
    )
```

```python
import functools

import jax
import jax.numpy as jnp
from jax import lax
from jax.experimental import pallas as pl
from jax.experimental.pallas import tpu as pltpu
from jax.sharding import PartitionSpec as P


tau_step = 0.25
prior_weight = 1.0


AXES = ("gx", "gy", "gz")
SLABS = ("gx", "gy")
ROWS = 5


def project_simplex(values, total):
    a, b, c, d = values
    a, b = jnp.maximum(a, b), jnp.minimum(a, b)
    c, d = jnp.maximum(c, d), jnp.minimum(c, d)
    a, c = jnp.maximum(a, c), jnp.minimum(a, c)
    b, d = jnp.maximum(b, d), jnp.minimum(b, d)
    b, c = jnp.maximum(b, c), jnp.minimum(b, c)
    one = a - total
    two = one + b
    three = two + c
    four = three + d
    threshold = jnp.maximum(
        jnp.maximum(one, two * 0.5), jnp.maximum(three * (1.0 / 3.0), four * 0.25)
    )
    return [jnp.maximum(value - threshold, 0.0) for value in values]


def affine(centers, unit):
    return [
        (center * (2.0 * unit * tau_step), center * center * (unit * tau_step))
        for center in centers
    ]


def attraction(volume, terms):
    return [volume * slope - offset for slope, offset in terms]


def shrink_of(x, y, z):
    return lax.rsqrt(jnp.maximum(x * x + y * y + z * z, 1.0))


class Planes:
    def __init__(self, shape, height, x_first, x_total):
        self.height = height
        self.rows, self.lanes = shape
        lane = lax.broadcasted_iota(jnp.int32, shape, 1)
        self.low = lane < height
        y = jnp.where(self.low, lane, lane - height)
        x = x_first + jnp.where(self.low, 0, 1)
        self.open_x = (x != x_total - 1).astype(jnp.float32)
        self.open_y = (y != height - 1).astype(jnp.float32)
        self.inside = (x >= 0).astype(jnp.float32)

    def dual(self, value, next_z, old=None):
        swapped = pltpu.roll(value, self.height, 1)
        following = jnp.where(self.low, swapped, pltpu.roll(swapped, self.rows - 1, 0))
        x = (following - value) * self.open_x
        y = (pltpu.roll(value, self.lanes - 1, 1) - value) * self.open_y
        z = next_z - value
        if old is not None:
            x, y, z = old[0] + x, old[1] + y, old[2] + z
        shrink = shrink_of(x, y, z)
        return x * shrink, y * shrink, z * shrink

    def behind_xy(self, x, y):
        swapped = pltpu.roll(x, self.height, 1)
        before_x = jnp.where(self.low, pltpu.roll(swapped, 1, 0), swapped)
        return (x - before_x) + (y - pltpu.roll(y, 1, 1))


def total_of(value):
    return jnp.sum(jnp.sum(value, axis=0, keepdims=True), axis=1, keepdims=True)


def base_kernel(levels_ref, base_ref):
    values = levels_ref[...].astype(jnp.float32) / 255.0
    for label in range(values.shape[1]):
        base_ref[label : label + 1] = jnp.broadcast_to(
            values[:, label : label + 1], (1, base_ref.shape[1])
        )


def base_of(base_ref):
    return [base_ref[label : label + 1] for label in range(base_ref.shape[0])]


def pack_sums(sums, shape):
    lane = lax.broadcasted_iota(jnp.int32, shape, 1)
    row = jnp.zeros(shape, jnp.float32)
    for index, value in enumerate(sums):
        row = jnp.where(lane == index, total_of(value), row)
    return row


def slab_index():
    return lax.axis_index("gx") * lax.axis_size("gy") + lax.axis_index("gy")


def open_lanes(depth):
    lane = lax.broadcasted_iota(jnp.int32, (1, depth), 1)
    return (lane != depth - 1).astype(jnp.float32)


def volume_layers(v_ref, pair_ref, other_ref, halo):
    thick = v_ref.shape[0]
    odd = lax.rem(slab_index(), 2) == 1

    def read(layer, rows=slice(None)):
        if layer < halo:
            layer += thick - halo
            return jnp.where(odd, pair_ref[layer, rows], other_ref[layer, rows])
        layer -= halo
        if layer < thick:
            return v_ref[layer, rows]
        layer -= thick
        return jnp.where(odd, other_ref[layer, rows], pair_ref[layer, rows])

    return read


def add_to(sums, index, term):
    sums[index] = term if sums[index] is None else sums[index] + term


CHUNK = 16
COVER = 50_000_000


def store_padded(ref, where, start, value, height):
    rows = value.shape[0]
    ref[where + (slice(start, start + rows),)] = value
    if start + rows == height:
        ref[where + (slice(height, height + 1),)] = value[rows - 1 :]


def first_halves(read, layers, height, terms, h_ref):
    for layer in layers:
        for start in range(0, height, CHUNK):
            values = read(layer, slice(start, start + CHUNK))
            for label, half in enumerate(project_simplex(attraction(values, terms), 0.5)):
                store_padded(h_ref, (label, layer), start, half, height)


def gradient(h_ref, label, layer, height, depth, open_z):
    half = h_ref[label, layer, 0:height]
    x = h_ref[label, layer + 1, 0:height] - half
    y = h_ref[label, layer, 1 : height + 1] - half
    z = (pltpu.roll(half, depth - 1, 1) - half) * open_z
    return x, y, z


def behind_yz(y, z, y_ref, where, height):
    y_ref[where + (slice(0, 8),)] = jnp.zeros((8, y.shape[1]), jnp.float32)
    y_ref[where + (slice(8, 8 + height),)] = y
    return (y - y_ref[where + (slice(7, 7 + height),)]) + (z - pltpu.roll(z, 1, 1))


def pair_kernel(v_ref, pair_ref, base_ref, h_ref, e_ref, sums_ref, planes_ref, y_ref, d_ref, b_ref):
    thick, height, depth = v_ref.shape
    lanes = thick * height
    labels = base_ref.shape[0]
    terms = affine(base_of(base_ref), 0.5)
    open_z = open_lanes(depth)
    odd = lax.rem(slab_index(), 2)
    sign = (1 - 2 * odd).astype(jnp.float32) * 0.0625
    even = (1 - odd).astype(jnp.float32) * 0.0625
    near = odd * (thick - 1)

    def read(layer, rows):
        return v_ref[layer, rows] if layer < thick else pair_ref[near, rows]

    first_halves(read, range(thick + 1), height, terms, h_ref)
    turned = jnp.transpose(v_ref[...].reshape(lanes, depth))
    planes_ref[0:2] = turned[0:2]
    planes_ref[2:4] = turned[depth - 2 : depth]
    at = jnp.where(odd == 1, 2, 1)
    following = jnp.where(odd == 1, 0, 2)
    done = 1 - odd
    for label in range(labels):
        for index, (layer, after) in enumerate(((0, 1), (at, following))):
            half = h_ref[label, layer, 0:height]
            x = h_ref[label, after, 0:height] - half
            y = h_ref[label, layer, 1 : height + 1] - half
            z = (pltpu.roll(half, depth - 1, 1) - half) * open_z
            shrink = shrink_of(x, y, z)
            d_ref[label, index] = x * shrink
            b_ref[label, index] = behind_yz(
                y * shrink, z * shrink, y_ref, (label, index), height
            )
    sums = [None] * (2 * labels)
    for start in range(0, height, CHUNK):
        rows = slice(start, start + CHUNK)
        values = v_ref[done, rows]
        entries = []
        for label, term in enumerate(attraction(values, terms)):
            across = sign * (d_ref[label, 1, rows] - d_ref[label, 0, rows])
            along = 0.0625 * b_ref[label, done, rows]
            entries.append(h_ref[label, done, rows] + term + (across + along))
        for label, value in enumerate(project_simplex(entries, 0.5)):
            add_to(sums, label, value)
            add_to(sums, labels + label, value * values)
        values = v_ref[odd, rows]
        for label, term in enumerate(attraction(values, terms)):
            part = sign * d_ref[label, 0, rows] + even * b_ref[label, 0, rows]
            e_ref[label, rows] = h_ref[label, odd, rows] + term + part
    for index, value in enumerate(sums):
        sums_ref[index] = value


def first_kernel(
    v_ref, other_ref, base_ref, h_ref, e_ref, sums_in, planes_ref, out_ref, n_ref, y_ref
):
    slabs = lax.axis_size(SLABS)
    blocks = lax.axis_size("gz")
    slab, block = slab_index(), lax.axis_index("gz")
    thick, height, depth = v_ref.shape
    lanes = thick * height
    devices = slabs * blocks
    labels = base_ref.shape[0]
    terms = affine(base_of(base_ref), 0.5)
    open_z = open_lanes(depth)
    odd = lax.rem(slab, 2)
    is_odd = odd == 1
    left = (1 - odd) * (thick - 1)

    for row in range(ROWS - 1):
        out_ref[pl.ds(row, devices, stride=ROWS), :] = jnp.broadcast_to(
            planes_ref[row : row + 1], (devices, lanes)
        )
    open_x = jnp.where(is_odd & (slab == slabs - 1), 0.0, 1.0)
    x_scale = jnp.where(is_odd, 0.0625, jnp.where(slab > 0, -0.0625, 0.0))
    yz_scale = jnp.where(is_odd, 0.0625, 0.0)
    for start in range(0, height, CHUNK):
        rows = slice(start, start + CHUNK)
        values = other_ref[left, rows]
        for label, half in enumerate(project_simplex(attraction(values, terms), 0.5)):
            known = h_ref[label, odd, rows]
            store_padded(n_ref, (label, 0), start, jnp.where(is_odd, known, half), height)
            n_ref[label, 1, rows] = jnp.where(is_odd, half, known)
    for label in range(labels):
        x, y, z = gradient(n_ref, label, 0, height, depth, open_z)
        x = x * open_x
        shrink = shrink_of(x, y, z)
        back = behind_yz(y * shrink, z * shrink, y_ref, (label,), height)
        n_ref[label, 1, 0:height] = x_scale * (x * shrink) + yz_scale * back
    sums = [sums_in[index] for index in range(2 * labels)]
    for start in range(0, height, CHUNK):
        rows = slice(start, start + CHUNK)
        values = v_ref[odd, rows]
        entries = [e_ref[label, rows] + n_ref[label, 1, rows] for label in range(labels)]
        for label, value in enumerate(project_simplex(entries, 0.5)):
            add_to(sums, label, value)
            add_to(sums, labels + label, value * values)
    lane = lax.broadcasted_iota(jnp.int32, (CHUNK, depth), 1)
    first = jnp.where(block > 0, 0, -1)
    last = jnp.where(block < blocks - 1, depth - 1, depth)
    keep = (lane != first) & (lane != last)
    sums = [jnp.where(keep, value, 0.0) for value in sums]
    out_ref[pl.ds(ROWS - 1, devices, stride=ROWS), :] = jnp.broadcast_to(
        pack_sums(sums, (1, lanes)), (devices, lanes)
    )


def ahead_kernel(
    v_ref, pair_ref, other_ref, base_ref, w_ref, q_ref, h_ref, s_ref, dual_ref, y_ref, l_ref
):
    slabs = lax.axis_size(SLABS)
    slab = slab_index()
    thick, height, depth = v_ref.shape
    lanes = thick * height
    labels = base_ref.shape[0]
    terms = affine(base_of(base_ref), 0.5)
    open_z = open_lanes(depth)
    halo = thick
    layers = thick + 2 * halo
    read = volume_layers(v_ref, pair_ref, other_ref, halo)

    first_halves(read, range(layers), height, terms, h_ref)
    inside = (slab > 0).astype(jnp.float32)
    open_x = (slab < slabs - 1).astype(jnp.float32)
    end = halo + thick - 1
    for label in range(labels):
        before = None
        for layer in range(layers - 1):
            x, y, z = gradient(h_ref, label, layer, height, depth, open_z)
            if layer == end:
                x = x * open_x
            shrink = shrink_of(x, y, z)
            x = x * shrink
            if layer == halo - 1:
                x = x * inside
            if layer:
                y, z = y * shrink, z * shrink
                where = (label, layer)
                dual_ref[label, 0, layer] = x
                dual_ref[label, 1, layer] = y
                dual_ref[label, 2, layer] = z
                l_ref[where] = (x - before) + behind_yz(y, z, y_ref, where, height)
            before = x
    for layer in range(1, layers - 1):
        for start in range(0, height, CHUNK):
            rows = slice(start, start + CHUNK)
            values = read(layer, rows)
            halves = [h_ref[label, layer, rows] for label in range(labels)]
            entries = [
                halves[label] + 0.0625 * l_ref[label, layer, rows] + term
                for label, term in enumerate(attraction(values, terms))
            ]
            for label, value in enumerate(project_simplex(entries, 0.5)):
                value = value + value
                store_padded(s_ref, (label, layer), start, value - halves[label], height)
                l_ref[label, layer, rows] = value
    for label in range(labels):
        before = None
        for layer in range(halo - 1, halo + thick):
            x, y, z = gradient(s_ref, label, layer, height, depth, open_z)
            if layer == end:
                x = x * open_x
            x = dual_ref[label, 0, layer] + x
            y = dual_ref[label, 1, layer] + y
            z = dual_ref[label, 2, layer] + z
            shrink = shrink_of(x, y, z)
            x = x * shrink
            if layer == halo - 1:
                x = x * inside
            else:
                divergence = (x - before) + behind_yz(
                    y * shrink, z * shrink, y_ref, (label, layer), height
                )
                w_ref[label, layer - halo] = l_ref[label, layer] + 0.125 * divergence
            before = x
    row = lax.broadcasted_iota(jnp.int32, (8, lanes), 0)
    near, far = [], []
    for start in (0, halo, halo + thick):
        turned = jnp.transpose(
            jnp.concatenate([read(start + index) for index in range(thick)], axis=0)
        )
        near.append(turned[0:8])
        far.append(turned[depth - 8 : depth])
    for column in range(6):
        plane = jnp.zeros((8, lanes), jnp.float32)
        for which in range(3):
            if column >= 2:
                plane = jnp.where(row == which, near[which][column - 2 : column - 1], plane)
            if column < 4:
                plane = jnp.where(row == 4 + which, far[which][4 + column : 5 + column], plane)
        q_ref[column] = plane


def last_kernel(v_ref, w_ref, q_ref, base_ref, got_ref, sums_ref, *rest):
    slabs = lax.axis_size(SLABS)
    blocks = lax.axis_size("gz")
    count = lax.axis_size("gy")
    slab, block = slab_index(), lax.axis_index("gz")
    pieces, lab_ref = rest[:count], rest[count]
    thick, height, depth = v_ref.shape
    lanes = thick * height
    labels = base_ref.shape[0]
    base = base_of(base_ref)
    terms = affine(base, 0.5)
    devices = slabs * blocks
    x_total = slabs * thick

    row = lax.broadcasted_iota(jnp.int32, (slabs, lanes), 0)
    everywhere = Planes((slabs, lanes), height, thick * row, x_total)
    sums = [None] * (2 * labels)
    for end in range(blocks - 1):
        planes = [
            got_ref[pl.ds((end + beyond) * ROWS + which, slabs, stride=blocks * ROWS), :]
            for beyond, which in ((0, 2), (0, 3), (1, 0), (1, 1))
        ]
        pulls = [attraction(plane, terms) for plane in planes]
        first = [project_simplex(pull, 0.5) for pull in pulls]
        divergence = [[], []]
        for label in range(labels):
            duals = [
                everywhere.dual(first[index][label], first[index + 1][label])
                for index in range(3)
            ]
            for index in (1, 2):
                x, y, z = duals[index]
                divergence[index - 1].append(
                    everywhere.behind_xy(x, y) + (z - duals[index - 1][2])
                )
        for index in (1, 2):
            entries = [
                first[index][label] + 0.0625 * divergence[index - 1][label] + pulls[index][label]
                for label in range(labels)
            ]
            for label, value in enumerate(project_simplex(entries, 0.5)):
                add_to(sums, label, value)
                add_to(sums, labels + label, value * planes[index])
    parts = got_ref[pl.ds(ROWS - 1, devices, stride=ROWS), :]
    lane = lax.broadcasted_iota(jnp.int32, (1, lanes), 1)
    parts = jnp.sum(parts, axis=0, keepdims=True)
    if blocks > 1:
        parts = parts + pack_sums(sums, (1, lanes))
    whole = [
        2.0 * jnp.sum(jnp.where(lane == index, parts, 0.0), axis=1, keepdims=True)
        for index in range(2 * labels)
    ]
    centers = [
        (whole[labels + label] + prior_weight * base[label]) / (whole[label] + prior_weight)
        for label in range(labels)
    ]

    row = lax.broadcasted_iota(jnp.int32, (8, lanes), 0)
    local = Planes((8, lanes), height, thick * (slab - 1 + (row & 3)), x_total)
    planes = [q_ref[column] for column in range(6)]
    for which in range(3):
        index = jnp.clip(slab - 1 + which, 0, slabs - 1) * blocks
        low = (index + jnp.maximum(block - 1, 0)) * ROWS
        high = (index + jnp.minimum(block + 1, blocks - 1)) * ROWS
        for column in range(2):
            source = got_ref[pl.ds(low + 2 + column, 1), :]
            planes[column] = jnp.where(row == which, source, planes[column])
            source = got_ref[pl.ds(high + column, 1), :]
            planes[4 + column] = jnp.where(row == 4 + which, source, planes[4 + column])
    pulls = [attraction(plane, terms) for plane in planes]
    first = [project_simplex(pull, 0.5) for pull in pulls]
    duals = []
    for label in range(labels):
        duals.append([])
        for column in range(5):
            x, y, z = local.dual(first[column][label], first[column + 1][label])
            duals[label].append((x * local.inside, y, z))
    second, smooth = {}, {}
    for column in range(1, 5):
        entries = []
        for label in range(labels):
            x, y, z = duals[label][column]
            divergence = local.behind_xy(x, y) + (z - duals[label][column - 1][2])
            entries.append(first[column][label] + 0.0625 * divergence + pulls[column][label])
        second[column] = [value + value for value in project_simplex(entries, 0.5)]
        smooth[column] = [
            second[column][label] - first[column][label] for label in range(labels)
        ]
    for label in range(labels):
        for column in range(1, 4):
            x, y, z = local.dual(
                smooth[column][label], smooth[column + 1][label], duals[label][column]
            )
            duals[label][column] = (x * local.inside, y, z)
    terms = affine(centers, 1.0)
    edge = {}
    for column in (2, 3):
        pull = attraction(planes[column], terms)
        entries = []
        for label in range(labels):
            x, y, z = duals[label][column]
            divergence = local.behind_xy(x, y) + (z - duals[label][column - 1][2])
            entries.append(second[column][label] + 0.125 * divergence + pull[label])
        edge[column] = project_simplex(entries, 1.0)
    step = depth // labels
    tiles = [jnp.zeros((8, lanes), jnp.float32) for _ in range(depth // 8)]
    for label in range(labels):
        two, three = edge[2][label], edge[3][label]
        place = label * step // 8
        tiles[place] = tiles[place] + jnp.where(
            row == 0, pltpu.roll(two, 7, 0), jnp.where(row == 1, three, 0.0)
        )
        place = (place - 1) % (depth // 8)
        tiles[place] = tiles[place] + jnp.where(
            row == 6, pltpu.roll(two, 1, 0), jnp.where(row == 7, pltpu.roll(three, 2, 0), 0.0)
        )
    columns = jnp.transpose(jnp.concatenate(tiles, axis=0))

    z = lax.broadcasted_iota(jnp.int32, (CHUNK, depth), 1)
    replaced = ((z < 2) & (block > 0)) | ((z >= depth - 2) & (block < blocks - 1))
    sums = [None] * (2 * labels)
    for layer in range(thick):
        for start in range(0, height, CHUNK):
            rows = slice(start, start + CHUNK)
            values = v_ref[layer, rows]
            entries = [
                w_ref[label, layer, rows] + pull
                for label, pull in enumerate(attraction(values, terms))
            ]
            for label, value in enumerate(project_simplex(entries, 1.0)):
                column = columns[layer * height + start : layer * height + start + CHUNK]
                if label:
                    column = pltpu.roll(column, depth - label * step, 1)
                value = jnp.where(replaced, column, value)
                lab_ref[label, layer, rows] = value
                add_to(sums, label, value)
                add_to(sums, labels + label, value * values)
    sums_ref[...] = jnp.broadcast_to(pack_sums(sums, (1, lanes)), (devices, lanes))
    rows = height // count
    me = lax.axis_index("gy")
    for other in range(count):
        start = pl.multiple_of((me ^ other) * rows, rows)
        pieces[other][...] = lab_ref[:, :, pl.ds(start, rows), :]


def join_kernel(*refs):
    *pieces, out_ref = refs
    me = lax.axis_index("gy")
    thick = pieces[0].shape[1]
    for other, piece in enumerate(pieces):
        out_ref[:, pl.ds((me ^ other) * thick, thick)] = piece[...]


def local(volume, levels):
    slabs = lax.axis_size(SLABS)
    blocks = lax.axis_size("gz")
    count = lax.axis_size("gy")
    devices = slabs * blocks
    thick, height, depth = volume.shape
    labels = levels.shape[0]
    lanes = thick * height
    if thick != 2 or labels != 4 or count & (count - 1):
        raise ValueError("unsupported sizes")
    f32 = functools.partial(jax.ShapeDtypeStruct, dtype=jnp.float32)
    vmem = pl.BlockSpec(memory_space=pltpu.VMEM)

    base_levels = levels.astype(jnp.float32) / 255.0
    params = pltpu.CompilerParams(vmem_limit_bytes=8 << 20)
    base = pl.pallas_call(
        base_kernel,
        out_shape=f32((labels, lanes)),
        in_specs=[vmem],
        out_specs=vmem,
        compiler_params=params,
        cost_estimate=pl.CostEstimate(flops=COVER, bytes_accessed=0, transcendentals=0),
        name="base",
    )(levels.reshape(1, labels))

    pairs = [(i, i ^ 1) for i in range(slabs)]
    across = [(i, i + 1) for i in range(1, slabs - 1, 2)]
    across += [(target, source) for source, target in across]
    pair = lax.ppermute(volume, SLABS, pairs)
    other = lax.ppermute(volume, SLABS, across)

    halves, entries, parts, edges = pl.pallas_call(
        pair_kernel,
        out_shape=[
            f32((labels, thick + 1, height + 8, depth)),
            f32((labels, height, depth)),
            f32((2 * labels, CHUNK, depth)),
            f32((4, lanes)),
        ],
        in_specs=[vmem] * 3,
        out_specs=[vmem] * 4,
        scratch_shapes=[
            pltpu.VMEM((labels, 2, height + 8, depth), jnp.float32),
            pltpu.VMEM((labels, 2, height, depth), jnp.float32),
            pltpu.VMEM((labels, 2, height, depth), jnp.float32),
        ],
        compiler_params=params,
        cost_estimate=pl.CostEstimate(flops=COVER, bytes_accessed=0, transcendentals=0),
        name="pair",
    )(volume, pair, base)
    sent = pl.pallas_call(
        first_kernel,
        out_shape=f32((devices * ROWS, lanes)),
        in_specs=[vmem] * 7,
        out_specs=vmem,
        scratch_shapes=[
            pltpu.VMEM((labels, 2, height + 8, depth), jnp.float32),
            pltpu.VMEM((labels, height + 8, depth), jnp.float32),
        ],
        compiler_params=params,
        name="first",
    )(volume, other, base, halves, entries, parts, edges)
    got = lax.all_to_all(sent.reshape(devices, 1, ROWS * lanes), AXES, 0, 0, tiled=True)
    got = got.reshape(devices * ROWS, lanes)

    layers = 3 * thick
    ahead, planes = pl.pallas_call(
        ahead_kernel,
        out_shape=[f32((labels, thick, height, depth)), f32((6, 8, lanes))],
        in_specs=[vmem] * 4,
        out_specs=[vmem] * 2,
        scratch_shapes=[
            pltpu.VMEM((labels, layers, height + 8, depth), jnp.float32),
            pltpu.VMEM((labels, layers, height + 8, depth), jnp.float32),
            pltpu.VMEM((labels, 3, layers, height, depth), jnp.float32),
            pltpu.VMEM((labels, layers, height + 8, depth), jnp.float32),
            pltpu.VMEM((labels, layers, height, depth), jnp.float32),
        ],
        cost_estimate=pl.CostEstimate(
            flops=200 * labels * layers * height * depth,
            bytes_accessed=4 * 20 * height * depth,
            transcendentals=0,
        ),
        compiler_params=params,
        name="ahead",
    )(volume, pair, other, base)

    piece = f32((labels, thick, height // count, depth))
    sums, *pieces = pl.pallas_call(
        last_kernel,
        out_shape=[f32((devices, lanes))] + [piece] * count,
        in_specs=[vmem] * 5,
        out_specs=[vmem] * (count + 1),
        scratch_shapes=[pltpu.VMEM((labels, thick, height, depth), jnp.float32)],
        compiler_params=params,
        name="last",
    )(volume, ahead, planes, base, got)

    total = lax.all_to_all(sums.reshape(devices, 1, lanes), AXES, 0, 0, tiled=True)
    for shift in range(1, count):
        pieces[shift] = lax.ppermute(pieces[shift], "gy", [(i, i ^ shift) for i in range(count)])
    join = pl.pallas_call(
        join_kernel,
        out_shape=f32((labels, thick * count, height // count, depth)),
        in_specs=[vmem] * count,
        out_specs=vmem,
        cost_estimate=pl.CostEstimate(
            flops=labels * thick * height * depth,
            bytes_accessed=8 * labels * thick * height * depth,
            transcendentals=0,
        ),
        compiler_params=params,
        name="join",
    )
    labelling = join(*pieces)
    total = total.sum((0, 1))
    sizes_all, weighted_all = total[:labels], total[labels : 2 * labels]
    centers = (weighted_all + prior_weight * base_levels) / (sizes_all + prior_weight)
    return (labelling, centers)


def solution(mesh):
    return jax.shard_map(
        local,
        mesh=mesh,
        in_specs=(P(("gx", "gy"), None, "gz"), P()),
        out_specs=(P(None, "gx", "gy", "gz"), P()),
        check_vma=False,
    )
```

```python
import functools

import jax
import jax.numpy as jnp
from jax import lax
from jax.experimental import pallas as pl
from jax.experimental.pallas import tpu as pltpu
from jax.sharding import PartitionSpec as P


tau_step = 0.25
prior_weight = 1.0


AXES = ("gy", "gx", "gz")
SLABS = ("gx", "gy")
ROWS = 5


def project_simplex(values, total):
    a, b, c, d = values
    a, b = jnp.maximum(a, b), jnp.minimum(a, b)
    c, d = jnp.maximum(c, d), jnp.minimum(c, d)
    a, c = jnp.maximum(a, c), jnp.minimum(a, c)
    b, d = jnp.maximum(b, d), jnp.minimum(b, d)
    b, c = jnp.maximum(b, c), jnp.minimum(b, c)
    one = a - total
    two = one + b
    three = two + c
    four = three + d
    threshold = jnp.maximum(
        jnp.maximum(one, two * 0.5), jnp.maximum(three * (1.0 / 3.0), four * 0.25)
    )
    return [jnp.maximum(value - threshold, 0.0) for value in values]


def affine(centers, unit):
    return [
        (center * (2.0 * unit * tau_step), center * center * (unit * tau_step))
        for center in centers
    ]


def attraction(volume, terms):
    return [volume * slope - offset for slope, offset in terms]


def shrink_of(x, y, z):
    return lax.rsqrt(jnp.maximum(x * x + y * y + z * z, 1.0))


class Planes:
    def __init__(self, shape, height, x_first, x_total):
        self.height = height
        self.rows, self.lanes = shape
        lane = lax.broadcasted_iota(jnp.int32, shape, 1)
        self.low = lane < height
        y = jnp.where(self.low, lane, lane - height)
        x = x_first + jnp.where(self.low, 0, 1)
        self.open_x = (x != x_total - 1).astype(jnp.float32)
        self.open_y = (y != height - 1).astype(jnp.float32)
        self.inside = (x >= 0).astype(jnp.float32)

    def dual(self, value, next_z, old=None):
        swapped = pltpu.roll(value, self.height, 1)
        following = jnp.where(self.low, swapped, pltpu.roll(swapped, self.rows - 1, 0))
        x = (following - value) * self.open_x
        y = (pltpu.roll(value, self.lanes - 1, 1) - value) * self.open_y
        z = next_z - value
        if old is not None:
            x, y, z = old[0] + x, old[1] + y, old[2] + z
        shrink = shrink_of(x, y, z)
        return x * shrink, y * shrink, z * shrink

    def behind_xy(self, x, y):
        swapped = pltpu.roll(x, self.height, 1)
        before_x = jnp.where(self.low, pltpu.roll(swapped, 1, 0), swapped)
        return (x - before_x) + (y - pltpu.roll(y, 1, 1))


def total_of(value):
    return jnp.sum(jnp.sum(value, axis=0, keepdims=True), axis=1, keepdims=True)


def base_kernel(levels_ref, base_ref):
    values = levels_ref[...].astype(jnp.float32) / 255.0
    for label in range(values.shape[1]):
        base_ref[label : label + 1] = jnp.broadcast_to(
            values[:, label : label + 1], (1, base_ref.shape[1])
        )


def base_of(base_ref):
    return [base_ref[label : label + 1] for label in range(base_ref.shape[0])]


def pack_sums(sums, shape):
    lane = lax.broadcasted_iota(jnp.int32, shape, 1)
    row = jnp.zeros(shape, jnp.float32)
    for index, value in enumerate(sums):
        row = jnp.where(lane == index, total_of(value), row)
    return row


def rank_of(slab):
    count = lax.axis_size("gy")
    return lax.rem(slab, count) * lax.axis_size("gx") + slab // count


def slab_index():
    return lax.axis_index("gx") * lax.axis_size("gy") + lax.axis_index("gy")


def open_lanes(depth):
    lane = lax.broadcasted_iota(jnp.int32, (1, depth), 1)
    return (lane != depth - 1).astype(jnp.float32)


def volume_layers(v_ref, pair_ref, other_ref, halo):
    thick = v_ref.shape[0]
    odd = lax.rem(slab_index(), 2) == 1

    def read(layer, rows=slice(None)):
        if layer < halo:
            layer += thick - halo
            return jnp.where(odd, pair_ref[layer, rows], other_ref[layer, rows])
        layer -= halo
        if layer < thick:
            return v_ref[layer, rows]
        layer -= thick
        return jnp.where(odd, other_ref[layer, rows], pair_ref[layer, rows])

    return read


def add_to(sums, index, term):
    sums[index] = term if sums[index] is None else sums[index] + term


CHUNK = 16
COVER = 50_000_000


def store_padded(ref, where, start, value, height):
    rows = value.shape[0]
    ref[where + (slice(start, start + rows),)] = value
    if start + rows == height:
        ref[where + (slice(height, height + 1),)] = value[rows - 1 :]


def first_halves(read, layers, height, terms, h_ref):
    for layer in layers:
        for start in range(0, height, CHUNK):
            values = read(layer, slice(start, start + CHUNK))
            for label, half in enumerate(project_simplex(attraction(values, terms), 0.5)):
                store_padded(h_ref, (label, layer), start, half, height)


def gradient(h_ref, label, layer, height, depth, open_z):
    half = h_ref[label, layer, 0:height]
    x = h_ref[label, layer + 1, 0:height] - half
    y = h_ref[label, layer, 1 : height + 1] - half
    z = (pltpu.roll(half, depth - 1, 1) - half) * open_z
    return x, y, z


def behind_yz(y, z, y_ref, where, height):
    y_ref[where + (slice(0, 8),)] = jnp.zeros((8, y.shape[1]), jnp.float32)
    y_ref[where + (slice(8, 8 + height),)] = y
    return (y - y_ref[where + (slice(7, 7 + height),)]) + (z - pltpu.roll(z, 1, 1))


def pair_kernel(v_ref, pair_ref, base_ref, h_ref, e_ref, sums_ref, planes_ref, y_ref, d_ref, b_ref):
    thick, height, depth = v_ref.shape
    lanes = thick * height
    labels = base_ref.shape[0]
    terms = affine(base_of(base_ref), 0.5)
    open_z = open_lanes(depth)
    odd = lax.rem(slab_index(), 2)
    sign = (1 - 2 * odd).astype(jnp.float32) * 0.0625
    even = (1 - odd).astype(jnp.float32) * 0.0625
    near = odd * (thick - 1)

    def read(layer, rows):
        return v_ref[layer, rows] if layer < thick else pair_ref[near, rows]

    first_halves(read, range(thick + 1), height, terms, h_ref)
    turned = jnp.transpose(v_ref[...].reshape(lanes, depth))
    planes_ref[0:2] = turned[0:2]
    planes_ref[2:4] = turned[depth - 2 : depth]
    at = jnp.where(odd == 1, 2, 1)
    following = jnp.where(odd == 1, 0, 2)
    done = 1 - odd
    for label in range(labels):
        for index, (layer, after) in enumerate(((0, 1), (at, following))):
            half = h_ref[label, layer, 0:height]
            x = h_ref[label, after, 0:height] - half
            y = h_ref[label, layer, 1 : height + 1] - half
            z = (pltpu.roll(half, depth - 1, 1) - half) * open_z
            shrink = shrink_of(x, y, z)
            d_ref[label, index] = x * shrink
            b_ref[label, index] = behind_yz(
                y * shrink, z * shrink, y_ref, (label, index), height
            )
    sums = [None] * (2 * labels)
    for start in range(0, height, CHUNK):
        rows = slice(start, start + CHUNK)
        values = v_ref[done, rows]
        entries = []
        for label, term in enumerate(attraction(values, terms)):
            across = sign * (d_ref[label, 1, rows] - d_ref[label, 0, rows])
            along = 0.0625 * b_ref[label, done, rows]
            entries.append(h_ref[label, done, rows] + term + (across + along))
        for label, value in enumerate(project_simplex(entries, 0.5)):
            add_to(sums, label, value)
            add_to(sums, labels + label, value * values)
        values = v_ref[odd, rows]
        for label, term in enumerate(attraction(values, terms)):
            part = sign * d_ref[label, 0, rows] + even * b_ref[label, 0, rows]
            e_ref[label, rows] = h_ref[label, odd, rows] + term + part
    for index, value in enumerate(sums):
        sums_ref[index] = value


def first_kernel(
    v_ref, other_ref, base_ref, h_ref, e_ref, sums_in, planes_ref, out_ref, n_ref, y_ref
):
    slabs = lax.axis_size(SLABS)
    blocks = lax.axis_size("gz")
    slab, block = slab_index(), lax.axis_index("gz")
    thick, height, depth = v_ref.shape
    lanes = thick * height
    devices = slabs * blocks
    labels = base_ref.shape[0]
    terms = affine(base_of(base_ref), 0.5)
    open_z = open_lanes(depth)
    odd = lax.rem(slab, 2)
    is_odd = odd == 1
    left = (1 - odd) * (thick - 1)

    for row in range(ROWS - 1):
        out_ref[pl.ds(row, devices, stride=ROWS), :] = jnp.broadcast_to(
            planes_ref[row : row + 1], (devices, lanes)
        )
    open_x = jnp.where(is_odd & (slab == slabs - 1), 0.0, 1.0)
    x_scale = jnp.where(is_odd, 0.0625, jnp.where(slab > 0, -0.0625, 0.0))
    yz_scale = jnp.where(is_odd, 0.0625, 0.0)
    for start in range(0, height, CHUNK):
        rows = slice(start, start + CHUNK)
        values = other_ref[left, rows]
        for label, half in enumerate(project_simplex(attraction(values, terms), 0.5)):
            known = h_ref[label, odd, rows]
            store_padded(n_ref, (label, 0), start, jnp.where(is_odd, known, half), height)
            n_ref[label, 1, rows] = jnp.where(is_odd, half, known)
    for label in range(labels):
        x, y, z = gradient(n_ref, label, 0, height, depth, open_z)
        x = x * open_x
        shrink = shrink_of(x, y, z)
        back = behind_yz(y * shrink, z * shrink, y_ref, (label,), height)
        n_ref[label, 1, 0:height] = x_scale * (x * shrink) + yz_scale * back
    sums = [sums_in[index] for index in range(2 * labels)]
    for start in range(0, height, CHUNK):
        rows = slice(start, start + CHUNK)
        values = v_ref[odd, rows]
        entries = [e_ref[label, rows] + n_ref[label, 1, rows] for label in range(labels)]
        for label, value in enumerate(project_simplex(entries, 0.5)):
            add_to(sums, label, value)
            add_to(sums, labels + label, value * values)
    lane = lax.broadcasted_iota(jnp.int32, (CHUNK, depth), 1)
    first = jnp.where(block > 0, 0, -1)
    last = jnp.where(block < blocks - 1, depth - 1, depth)
    keep = (lane != first) & (lane != last)
    sums = [jnp.where(keep, value, 0.0) for value in sums]
    out_ref[pl.ds(ROWS - 1, devices, stride=ROWS), :] = jnp.broadcast_to(
        pack_sums(sums, (1, lanes)), (devices, lanes)
    )


def ahead_kernel(
    v_ref, pair_ref, other_ref, base_ref, w_ref, q_ref, h_ref, s_ref, dual_ref, y_ref, l_ref
):
    slabs = lax.axis_size(SLABS)
    slab = slab_index()
    thick, height, depth = v_ref.shape
    lanes = thick * height
    labels = base_ref.shape[0]
    terms = affine(base_of(base_ref), 0.5)
    open_z = open_lanes(depth)
    halo = thick
    layers = thick + 2 * halo
    read = volume_layers(v_ref, pair_ref, other_ref, halo)

    first_halves(read, range(layers), height, terms, h_ref)
    inside = (slab > 0).astype(jnp.float32)
    open_x = (slab < slabs - 1).astype(jnp.float32)
    end = halo + thick - 1
    for label in range(labels):
        before = None
        for layer in range(layers - 1):
            x, y, z = gradient(h_ref, label, layer, height, depth, open_z)
            if layer == end:
                x = x * open_x
            shrink = shrink_of(x, y, z)
            x = x * shrink
            if layer == halo - 1:
                x = x * inside
            if layer:
                y, z = y * shrink, z * shrink
                where = (label, layer)
                dual_ref[label, 0, layer] = x
                dual_ref[label, 1, layer] = y
                dual_ref[label, 2, layer] = z
                l_ref[where] = (x - before) + behind_yz(y, z, y_ref, where, height)
            before = x
    for layer in range(1, layers - 1):
        for start in range(0, height, CHUNK):
            rows = slice(start, start + CHUNK)
            values = read(layer, rows)
            halves = [h_ref[label, layer, rows] for label in range(labels)]
            entries = [
                halves[label] + 0.0625 * l_ref[label, layer, rows] + term
                for label, term in enumerate(attraction(values, terms))
            ]
            for label, value in enumerate(project_simplex(entries, 0.5)):
                value = value + value
                store_padded(s_ref, (label, layer), start, value - halves[label], height)
                l_ref[label, layer, rows] = value
    for label in range(labels):
        before = None
        for layer in range(halo - 1, halo + thick):
            x, y, z = gradient(s_ref, label, layer, height, depth, open_z)
            if layer == end:
                x = x * open_x
            x = dual_ref[label, 0, layer] + x
            y = dual_ref[label, 1, layer] + y
            z = dual_ref[label, 2, layer] + z
            shrink = shrink_of(x, y, z)
            x = x * shrink
            if layer == halo - 1:
                x = x * inside
            else:
                divergence = (x - before) + behind_yz(
                    y * shrink, z * shrink, y_ref, (label, layer), height
                )
                w_ref[label, layer - halo] = l_ref[label, layer] + 0.125 * divergence
            before = x
    row = lax.broadcasted_iota(jnp.int32, (8, lanes), 0)
    near, far = [], []
    for start in (0, halo, halo + thick):
        turned = jnp.transpose(
            jnp.concatenate([read(start + index) for index in range(thick)], axis=0)
        )
        near.append(turned[0:8])
        far.append(turned[depth - 8 : depth])
    for column in range(6):
        plane = jnp.zeros((8, lanes), jnp.float32)
        for which in range(3):
            if column >= 2:
                plane = jnp.where(row == which, near[which][column - 2 : column - 1], plane)
            if column < 4:
                plane = jnp.where(row == 4 + which, far[which][4 + column : 5 + column], plane)
        q_ref[column] = plane


def last_kernel(v_ref, w_ref, q_ref, base_ref, got_ref, sums_ref, *rest):
    slabs = lax.axis_size(SLABS)
    blocks = lax.axis_size("gz")
    count = lax.axis_size("gy")
    groups = lax.axis_size("gx")
    slab, block = slab_index(), lax.axis_index("gz")
    pieces, lab_ref = rest[:count], rest[count]
    thick, height, depth = v_ref.shape
    lanes = thick * height
    labels = base_ref.shape[0]
    base = base_of(base_ref)
    terms = affine(base, 0.5)
    devices = slabs * blocks
    x_total = slabs * thick

    row = lax.broadcasted_iota(jnp.int32, (slabs, lanes), 0)
    everywhere = Planes((slabs, lanes), height, thick * row, x_total)
    sums = [None] * (2 * labels)
    for end in range(blocks - 1):
        planes = []
        for beyond, which in ((0, 2), (0, 3), (1, 0), (1, 1)):
            start = (end + beyond) * ROWS + which
            planes.append(
                jnp.concatenate(
                    [
                        got_ref[
                            pl.ds(start + outer * blocks * ROWS, count, stride=groups * blocks * ROWS)
                        ]
                        for outer in range(groups)
                    ],
                    axis=0,
                )
            )
        pulls = [attraction(plane, terms) for plane in planes]
        first = [project_simplex(pull, 0.5) for pull in pulls]
        divergence = [[], []]
        for label in range(labels):
            duals = [
                everywhere.dual(first[index][label], first[index + 1][label])
                for index in range(3)
            ]
            for index in (1, 2):
                x, y, z = duals[index]
                divergence[index - 1].append(
                    everywhere.behind_xy(x, y) + (z - duals[index - 1][2])
                )
        for index in (1, 2):
            entries = [
                first[index][label] + 0.0625 * divergence[index - 1][label] + pulls[index][label]
                for label in range(labels)
            ]
            for label, value in enumerate(project_simplex(entries, 0.5)):
                add_to(sums, label, value)
                add_to(sums, labels + label, value * planes[index])
    parts = got_ref[pl.ds(ROWS - 1, devices, stride=ROWS), :]
    lane = lax.broadcasted_iota(jnp.int32, (1, lanes), 1)
    parts = jnp.sum(parts, axis=0, keepdims=True)
    whole = []
    for index in range(2 * labels):
        part = jnp.where(lane == index, parts, 0.0)
        if blocks > 1:
            part = part + jnp.sum(sums[index], axis=0, keepdims=True)
        whole.append(2.0 * jnp.sum(part, axis=1, keepdims=True))
    centers = [
        (whole[labels + label] + prior_weight * base[label]) / (whole[label] + prior_weight)
        for label in range(labels)
    ]

    row = lax.broadcasted_iota(jnp.int32, (8, lanes), 0)
    local = Planes((8, lanes), height, thick * (slab - 1 + (row & 3)), x_total)
    planes = [q_ref[column] for column in range(6)]
    for which in range(3):
        index = rank_of(jnp.clip(slab - 1 + which, 0, slabs - 1)) * blocks
        low = (index + jnp.maximum(block - 1, 0)) * ROWS
        high = (index + jnp.minimum(block + 1, blocks - 1)) * ROWS
        for column in range(2):
            source = got_ref[pl.ds(low + 2 + column, 1), :]
            planes[column] = jnp.where(row == which, source, planes[column])
            source = got_ref[pl.ds(high + column, 1), :]
            planes[4 + column] = jnp.where(row == 4 + which, source, planes[4 + column])
    pulls = [attraction(plane, terms) for plane in planes]
    first = [project_simplex(pull, 0.5) for pull in pulls]
    duals = []
    for label in range(labels):
        duals.append([])
        for column in range(5):
            x, y, z = local.dual(first[column][label], first[column + 1][label])
            duals[label].append((x * local.inside, y, z))
    second, smooth = {}, {}
    for column in range(1, 5):
        entries = []
        for label in range(labels):
            x, y, z = duals[label][column]
            divergence = local.behind_xy(x, y) + (z - duals[label][column - 1][2])
            entries.append(first[column][label] + 0.0625 * divergence + pulls[column][label])
        second[column] = [value + value for value in project_simplex(entries, 0.5)]
        smooth[column] = [
            second[column][label] - first[column][label] for label in range(labels)
        ]
    for label in range(labels):
        for column in range(1, 4):
            x, y, z = local.dual(
                smooth[column][label], smooth[column + 1][label], duals[label][column]
            )
            duals[label][column] = (x * local.inside, y, z)
    terms = affine(centers, 1.0)
    edge = {}
    for column in (2, 3):
        pull = attraction(planes[column], terms)
        entries = []
        for label in range(labels):
            x, y, z = duals[label][column]
            divergence = local.behind_xy(x, y) + (z - duals[label][column - 1][2])
            entries.append(second[column][label] + 0.125 * divergence + pull[label])
        edge[column] = project_simplex(entries, 1.0)
    step = depth // labels
    tiles = [jnp.zeros((8, lanes), jnp.float32) for _ in range(depth // 8)]
    for label in range(labels):
        two, three = edge[2][label], edge[3][label]
        place = label * step // 8
        tiles[place] = tiles[place] + jnp.where(
            row == 0, pltpu.roll(two, 7, 0), jnp.where(row == 1, three, 0.0)
        )
        place = (place - 1) % (depth // 8)
        tiles[place] = tiles[place] + jnp.where(
            row == 6, pltpu.roll(two, 1, 0), jnp.where(row == 7, pltpu.roll(three, 2, 0), 0.0)
        )
    columns = jnp.transpose(jnp.concatenate(tiles, axis=0))

    z = lax.broadcasted_iota(jnp.int32, (CHUNK, depth), 1)
    replaced = ((z < 2) & (block > 0)) | ((z >= depth - 2) & (block < blocks - 1))
    sums = [None] * (2 * labels)
    for layer in range(thick):
        for start in range(0, height, CHUNK):
            rows = slice(start, start + CHUNK)
            values = v_ref[layer, rows]
            entries = [
                w_ref[label, layer, rows] + pull
                for label, pull in enumerate(attraction(values, terms))
            ]
            for label, value in enumerate(project_simplex(entries, 1.0)):
                column = columns[layer * height + start : layer * height + start + CHUNK]
                if label:
                    column = pltpu.roll(column, depth - label * step, 1)
                value = jnp.where(replaced, column, value)
                lab_ref[label, layer, rows] = value
                add_to(sums, label, value)
                add_to(sums, labels + label, value * values)
    sums_ref[...] = jnp.broadcast_to(pack_sums(sums, (1, lanes)), (devices, lanes))
    rows = height // count
    me = lax.axis_index("gy")
    for other in range(count):
        start = pl.multiple_of((me ^ other) * rows, rows)
        pieces[other][...] = lab_ref[:, :, pl.ds(start, rows), :]


def join_kernel(*refs):
    *pieces, out_ref = refs
    me = lax.axis_index("gy")
    thick = pieces[0].shape[1]
    for other, piece in enumerate(pieces):
        out_ref[:, pl.ds((me ^ other) * thick, thick)] = piece[...]


def local(volume, levels):
    slabs = lax.axis_size(SLABS)
    blocks = lax.axis_size("gz")
    count = lax.axis_size("gy")
    devices = slabs * blocks
    thick, height, depth = volume.shape
    labels = levels.shape[0]
    lanes = thick * height
    if thick != 2 or labels != 4 or count & (count - 1):
        raise ValueError("unsupported sizes")
    f32 = functools.partial(jax.ShapeDtypeStruct, dtype=jnp.float32)
    vmem = pl.BlockSpec(memory_space=pltpu.VMEM)

    base_levels = levels.astype(jnp.float32) / 255.0
    params = pltpu.CompilerParams(vmem_limit_bytes=8 << 20)
    base = pl.pallas_call(
        base_kernel,
        out_shape=f32((labels, lanes)),
        in_specs=[vmem],
        out_specs=vmem,
        compiler_params=params,
        cost_estimate=pl.CostEstimate(flops=COVER, bytes_accessed=0, transcendentals=0),
        name="base",
    )(levels.reshape(1, labels))

    pairs = [(i, i ^ 1) for i in range(slabs)]
    across = [(i, (i + 1) % slabs) for i in range(1, slabs, 2)]
    across += [(target, source) for source, target in across]
    pair = lax.ppermute(volume, SLABS, pairs)
    other = lax.ppermute(volume, SLABS, across)

    halves, entries, parts, edges = pl.pallas_call(
        pair_kernel,
        out_shape=[
            f32((labels, thick + 1, height + 8, depth)),
            f32((labels, height, depth)),
            f32((2 * labels, CHUNK, depth)),
            f32((4, lanes)),
        ],
        in_specs=[vmem] * 3,
        out_specs=[vmem] * 4,
        scratch_shapes=[
            pltpu.VMEM((labels, 2, height + 8, depth), jnp.float32),
            pltpu.VMEM((labels, 2, height, depth), jnp.float32),
            pltpu.VMEM((labels, 2, height, depth), jnp.float32),
        ],
        compiler_params=params,
        cost_estimate=pl.CostEstimate(flops=COVER, bytes_accessed=0, transcendentals=0),
        name="pair",
    )(volume, pair, base)
    sent = pl.pallas_call(
        first_kernel,
        out_shape=f32((devices * ROWS, lanes)),
        in_specs=[vmem] * 7,
        out_specs=vmem,
        scratch_shapes=[
            pltpu.VMEM((labels, 2, height + 8, depth), jnp.float32),
            pltpu.VMEM((labels, height + 8, depth), jnp.float32),
        ],
        compiler_params=params,
        name="first",
    )(volume, other, base, halves, entries, parts, edges)
    got = lax.all_to_all(sent.reshape(devices, 1, ROWS * lanes), AXES, 0, 0, tiled=True)
    got = got.reshape(devices * ROWS, lanes)

    layers = 3 * thick
    ahead, planes = pl.pallas_call(
        ahead_kernel,
        out_shape=[f32((labels, thick, height, depth)), f32((6, 8, lanes))],
        in_specs=[vmem] * 4,
        out_specs=[vmem] * 2,
        scratch_shapes=[
            pltpu.VMEM((labels, layers, height + 8, depth), jnp.float32),
            pltpu.VMEM((labels, layers, height + 8, depth), jnp.float32),
            pltpu.VMEM((labels, 3, layers, height, depth), jnp.float32),
            pltpu.VMEM((labels, layers, height + 8, depth), jnp.float32),
            pltpu.VMEM((labels, layers, height, depth), jnp.float32),
        ],
        cost_estimate=pl.CostEstimate(
            flops=200 * labels * layers * height * depth,
            bytes_accessed=4 * 20 * height * depth,
            transcendentals=0,
        ),
        compiler_params=params,
        name="ahead",
    )(volume, pair, other, base)

    piece = f32((labels, thick, height // count, depth))
    sums, *pieces = pl.pallas_call(
        last_kernel,
        out_shape=[f32((devices, lanes))] + [piece] * count,
        in_specs=[vmem] * 5,
        out_specs=[vmem] * (count + 1),
        scratch_shapes=[pltpu.VMEM((labels, thick, height, depth), jnp.float32)],
        compiler_params=params,
        name="last",
    )(volume, ahead, planes, base, got)

    total = lax.all_to_all(sums.reshape(devices, 1, lanes), AXES, 0, 0, tiled=True)
    for shift in range(1, count):
        pieces[shift] = lax.ppermute(pieces[shift], "gy", [(i, i ^ shift) for i in range(count)])
    join = pl.pallas_call(
        join_kernel,
        out_shape=f32((labels, thick * count, height // count, depth)),
        in_specs=[vmem] * count,
        out_specs=vmem,
        cost_estimate=pl.CostEstimate(
            flops=labels * thick * height * depth,
            bytes_accessed=8 * labels * thick * height * depth,
            transcendentals=0,
        ),
        compiler_params=params,
        name="join",
    )
    labelling = join(*pieces)
    total = total.sum((0, 1))
    sizes_all, weighted_all = total[:labels], total[labels : 2 * labels]
    centers = (weighted_all + prior_weight * base_levels) / (sizes_all + prior_weight)
    return (labelling, centers)


def solution(mesh):
    return jax.shard_map(
        local,
        mesh=mesh,
        in_specs=(P(("gx", "gy"), None, "gz"), P()),
        out_specs=(P(None, "gx", "gy", "gz"), P()),
        check_vma=False,
    )
```

```python
import functools

import jax
import jax.numpy as jnp
from jax import lax
from jax.experimental import pallas as pl
from jax.experimental.pallas import tpu as pltpu
from jax.sharding import PartitionSpec as P


tau_step = 0.25
prior_weight = 1.0


AXES = ("gy", "gx", "gz")
SLABS = ("gx", "gy")
ROWS = 5


def project_simplex(values, total):
    a, b, c, d = values
    a, b = jnp.maximum(a, b), jnp.minimum(a, b)
    c, d = jnp.maximum(c, d), jnp.minimum(c, d)
    a, c = jnp.maximum(a, c), jnp.minimum(a, c)
    b, d = jnp.maximum(b, d), jnp.minimum(b, d)
    b, c = jnp.maximum(b, c), jnp.minimum(b, c)
    one = a - total
    two = one + b
    three = two + c
    four = three + d
    threshold = jnp.maximum(
        jnp.maximum(one, two * 0.5), jnp.maximum(three * (1.0 / 3.0), four * 0.25)
    )
    return [jnp.maximum(value - threshold, 0.0) for value in values]


def affine(centers, unit):
    return [
        (center * (2.0 * unit * tau_step), center * center * (unit * tau_step))
        for center in centers
    ]


def attraction(volume, terms):
    return [volume * slope - offset for slope, offset in terms]


def shrink_of(x, y, z):
    return lax.rsqrt(jnp.maximum(x * x + y * y + z * z, 1.0))


class Planes:
    def __init__(self, shape, height, x_first, x_total):
        self.height = height
        self.rows, self.lanes = shape
        lane = lax.broadcasted_iota(jnp.int32, shape, 1)
        self.low = lane < height
        y = jnp.where(self.low, lane, lane - height)
        x = x_first + jnp.where(self.low, 0, 1)
        self.open_x = (x != x_total - 1).astype(jnp.float32)
        self.open_y = (y != height - 1).astype(jnp.float32)
        self.inside = (x >= 0).astype(jnp.float32)

    def dual(self, value, next_z, old=None):
        swapped = pltpu.roll(value, self.height, 1)
        following = jnp.where(self.low, swapped, pltpu.roll(swapped, self.rows - 1, 0))
        x = (following - value) * self.open_x
        y = (pltpu.roll(value, self.lanes - 1, 1) - value) * self.open_y
        z = next_z - value
        if old is not None:
            x, y, z = old[0] + x, old[1] + y, old[2] + z
        shrink = shrink_of(x, y, z)
        return x * shrink, y * shrink, z * shrink

    def behind_xy(self, x, y):
        swapped = pltpu.roll(x, self.height, 1)
        before_x = jnp.where(self.low, pltpu.roll(swapped, 1, 0), swapped)
        return (x - before_x) + (y - pltpu.roll(y, 1, 1))


def total_of(value):
    return jnp.sum(jnp.sum(value, axis=0, keepdims=True), axis=1, keepdims=True)


def base_kernel(levels_ref, base_ref):
    values = levels_ref[...].astype(jnp.float32) / 255.0
    for label in range(values.shape[1]):
        base_ref[label : label + 1] = jnp.broadcast_to(
            values[:, label : label + 1], (1, base_ref.shape[1])
        )


def base_of(base_ref):
    return [base_ref[label : label + 1] for label in range(base_ref.shape[0])]


def pack_sums(sums, shape):
    lane = lax.broadcasted_iota(jnp.int32, shape, 1)
    row = jnp.zeros(shape, jnp.float32)
    for index, value in enumerate(sums):
        row = jnp.where(lane == index, total_of(value), row)
    return row


def rank_of(slab):
    count = lax.axis_size("gy")
    return lax.rem(slab, count) * lax.axis_size("gx") + slab // count


def slab_index():
    return lax.axis_index("gx") * lax.axis_size("gy") + lax.axis_index("gy")


def open_lanes(depth):
    lane = lax.broadcasted_iota(jnp.int32, (1, depth), 1)
    return (lane != depth - 1).astype(jnp.float32)


def volume_layers(v_ref, pair_ref, other_ref, halo):
    thick = v_ref.shape[0]
    odd = lax.rem(slab_index(), 2) == 1

    def read(layer, rows=slice(None)):
        if layer < halo:
            layer += thick - halo
            return jnp.where(odd, pair_ref[layer, rows], other_ref[layer, rows])
        layer -= halo
        if layer < thick:
            return v_ref[layer, rows]
        layer -= thick
        return jnp.where(odd, other_ref[layer, rows], pair_ref[layer, rows])

    return read


def add_to(sums, index, term):
    sums[index] = term if sums[index] is None else sums[index] + term


CHUNK = 16
COVER = 50_000_000


def store_padded(ref, where, start, value, height):
    rows = value.shape[0]
    ref[where + (slice(start, start + rows),)] = value
    if start + rows == height:
        ref[where + (slice(height, height + 1),)] = value[rows - 1 :]


def first_halves(read, layers, height, terms, h_ref):
    for layer in layers:
        for start in range(0, height, CHUNK):
            values = read(layer, slice(start, start + CHUNK))
            for label, half in enumerate(project_simplex(attraction(values, terms), 0.5)):
                store_padded(h_ref, (label, layer), start, half, height)


def gradient(h_ref, label, layer, height, depth, open_z):
    half = h_ref[label, layer, 0:height]
    x = h_ref[label, layer + 1, 0:height] - half
    y = h_ref[label, layer, 1 : height + 1] - half
    z = (pltpu.roll(half, depth - 1, 1) - half) * open_z
    return x, y, z


def behind_yz(y, z, y_ref, where, height):
    y_ref[where + (slice(0, 8),)] = jnp.zeros((8, y.shape[1]), jnp.float32)
    y_ref[where + (slice(8, 8 + height),)] = y
    return (y - y_ref[where + (slice(7, 7 + height),)]) + (z - pltpu.roll(z, 1, 1))


def pair_kernel(v_ref, pair_ref, base_ref, h_ref, e_ref, sums_ref, planes_ref, y_ref, d_ref, b_ref):
    thick, height, depth = v_ref.shape
    lanes = thick * height
    labels = base_ref.shape[0]
    terms = affine(base_of(base_ref), 0.5)
    open_z = open_lanes(depth)
    odd = lax.rem(slab_index(), 2)
    sign = (1 - 2 * odd).astype(jnp.float32) * 0.0625
    even = (1 - odd).astype(jnp.float32) * 0.0625
    near = odd * (thick - 1)

    def read(layer, rows):
        return v_ref[layer, rows] if layer < thick else pair_ref[near, rows]

    first_halves(read, range(thick + 1), height, terms, h_ref)
    turned = jnp.transpose(v_ref[...].reshape(lanes, depth))
    planes_ref[0:2] = turned[0:2]
    planes_ref[2:4] = turned[depth - 2 : depth]
    at = jnp.where(odd == 1, 2, 1)
    following = jnp.where(odd == 1, 0, 2)
    done = 1 - odd
    for label in range(labels):
        for index, (layer, after) in enumerate(((0, 1), (at, following))):
            half = h_ref[label, layer, 0:height]
            x = h_ref[label, after, 0:height] - half
            y = h_ref[label, layer, 1 : height + 1] - half
            z = (pltpu.roll(half, depth - 1, 1) - half) * open_z
            shrink = shrink_of(x, y, z)
            d_ref[label, index] = x * shrink
            b_ref[label, index] = behind_yz(
                y * shrink, z * shrink, y_ref, (label, index), height
            )
    sums = [None] * (2 * labels)
    for start in range(0, height, CHUNK):
        rows = slice(start, start + CHUNK)
        values = v_ref[done, rows]
        entries = []
        for label, term in enumerate(attraction(values, terms)):
            across = sign * (d_ref[label, 1, rows] - d_ref[label, 0, rows])
            along = 0.0625 * b_ref[label, done, rows]
            entries.append(h_ref[label, done, rows] + term + (across + along))
        for label, value in enumerate(project_simplex(entries, 0.5)):
            add_to(sums, label, value)
            add_to(sums, labels + label, value * values)
        values = v_ref[odd, rows]
        for label, term in enumerate(attraction(values, terms)):
            part = sign * d_ref[label, 0, rows] + even * b_ref[label, 0, rows]
            e_ref[label, rows] = h_ref[label, odd, rows] + term + part
    for index, value in enumerate(sums):
        sums_ref[index] = value


def first_kernel(
    v_ref, other_ref, base_ref, h_ref, e_ref, sums_in, planes_ref, out_ref, n_ref, y_ref
):
    slabs = lax.axis_size(SLABS)
    blocks = lax.axis_size("gz")
    slab, block = slab_index(), lax.axis_index("gz")
    thick, height, depth = v_ref.shape
    lanes = thick * height
    devices = slabs * blocks
    labels = base_ref.shape[0]
    terms = affine(base_of(base_ref), 0.5)
    open_z = open_lanes(depth)
    odd = lax.rem(slab, 2)
    is_odd = odd == 1
    left = (1 - odd) * (thick - 1)

    for row in range(ROWS - 1):
        out_ref[pl.ds(row, devices, stride=ROWS), :] = jnp.broadcast_to(
            planes_ref[row : row + 1], (devices, lanes)
        )
    open_x = jnp.where(is_odd & (slab == slabs - 1), 0.0, 1.0)
    x_scale = jnp.where(is_odd, 0.0625, jnp.where(slab > 0, -0.0625, 0.0))
    yz_scale = jnp.where(is_odd, 0.0625, 0.0)
    for start in range(0, height, CHUNK):
        rows = slice(start, start + CHUNK)
        values = other_ref[left, rows]
        for label, half in enumerate(project_simplex(attraction(values, terms), 0.5)):
            known = h_ref[label, odd, rows]
            store_padded(n_ref, (label, 0), start, jnp.where(is_odd, known, half), height)
            n_ref[label, 1, rows] = jnp.where(is_odd, half, known)
    for label in range(labels):
        x, y, z = gradient(n_ref, label, 0, height, depth, open_z)
        x = x * open_x
        shrink = shrink_of(x, y, z)
        back = behind_yz(y * shrink, z * shrink, y_ref, (label,), height)
        n_ref[label, 1, 0:height] = x_scale * (x * shrink) + yz_scale * back
    sums = [sums_in[index] for index in range(2 * labels)]
    for start in range(0, height, CHUNK):
        rows = slice(start, start + CHUNK)
        values = v_ref[odd, rows]
        entries = [e_ref[label, rows] + n_ref[label, 1, rows] for label in range(labels)]
        for label, value in enumerate(project_simplex(entries, 0.5)):
            add_to(sums, label, value)
            add_to(sums, labels + label, value * values)
    lane = lax.broadcasted_iota(jnp.int32, (CHUNK, depth), 1)
    first = jnp.where(block > 0, 0, -1)
    last = jnp.where(block < blocks - 1, depth - 1, depth)
    keep = (lane != first) & (lane != last)
    sums = [jnp.where(keep, value, 0.0) for value in sums]
    out_ref[pl.ds(ROWS - 1, devices, stride=ROWS), :] = jnp.broadcast_to(
        pack_sums(sums, (1, lanes)), (devices, lanes)
    )


def ahead_kernel(
    v_ref, pair_ref, other_ref, base_ref, w_ref, q_ref, h_ref, s_ref, dual_ref, y_ref, l_ref
):
    slabs = lax.axis_size(SLABS)
    slab = slab_index()
    thick, height, depth = v_ref.shape
    lanes = thick * height
    labels = base_ref.shape[0]
    terms = affine(base_of(base_ref), 0.5)
    open_z = open_lanes(depth)
    halo = thick
    layers = thick + 2 * halo
    read = volume_layers(v_ref, pair_ref, other_ref, halo)

    first_halves(read, range(layers), height, terms, h_ref)
    inside = (slab > 0).astype(jnp.float32)
    open_x = (slab < slabs - 1).astype(jnp.float32)
    end = halo + thick - 1
    for label in range(labels):
        before = None
        for layer in range(layers - 1):
            x, y, z = gradient(h_ref, label, layer, height, depth, open_z)
            if layer == end:
                x = x * open_x
            shrink = shrink_of(x, y, z)
            x = x * shrink
            if layer == halo - 1:
                x = x * inside
            if layer:
                y, z = y * shrink, z * shrink
                where = (label, layer)
                dual_ref[label, 0, layer] = x
                dual_ref[label, 1, layer] = y
                dual_ref[label, 2, layer] = z
                l_ref[where] = (x - before) + behind_yz(y, z, y_ref, where, height)
            before = x
    for layer in range(1, layers - 1):
        for start in range(0, height, CHUNK):
            rows = slice(start, start + CHUNK)
            values = read(layer, rows)
            halves = [h_ref[label, layer, rows] for label in range(labels)]
            entries = [
                halves[label] + 0.0625 * l_ref[label, layer, rows] + term
                for label, term in enumerate(attraction(values, terms))
            ]
            for label, value in enumerate(project_simplex(entries, 0.5)):
                value = value + value
                store_padded(s_ref, (label, layer), start, value - halves[label], height)
                l_ref[label, layer, rows] = value
    for label in range(labels):
        before = None
        for layer in range(halo - 1, halo + thick):
            x, y, z = gradient(s_ref, label, layer, height, depth, open_z)
            if layer == end:
                x = x * open_x
            x = dual_ref[label, 0, layer] + x
            y = dual_ref[label, 1, layer] + y
            z = dual_ref[label, 2, layer] + z
            shrink = shrink_of(x, y, z)
            x = x * shrink
            if layer == halo - 1:
                x = x * inside
            else:
                divergence = (x - before) + behind_yz(
                    y * shrink, z * shrink, y_ref, (label, layer), height
                )
                w_ref[label, layer - halo] = l_ref[label, layer] + 0.125 * divergence
            before = x
    row = lax.broadcasted_iota(jnp.int32, (8, lanes), 0)
    near, far = [], []
    for start in (0, halo, halo + thick):
        turned = jnp.transpose(
            jnp.concatenate([read(start + index) for index in range(thick)], axis=0)
        )
        near.append(turned[0:8])
        far.append(turned[depth - 8 : depth])
    for column in range(6):
        plane = jnp.zeros((8, lanes), jnp.float32)
        for which in range(3):
            if column >= 2:
                plane = jnp.where(row == which, near[which][column - 2 : column - 1], plane)
            if column < 4:
                plane = jnp.where(row == 4 + which, far[which][4 + column : 5 + column], plane)
        q_ref[column] = plane


def last_kernel(v_ref, w_ref, q_ref, base_ref, got_ref, sums_ref, *rest):
    slabs = lax.axis_size(SLABS)
    blocks = lax.axis_size("gz")
    count = lax.axis_size("gy")
    groups = lax.axis_size("gx")
    slab, block = slab_index(), lax.axis_index("gz")
    pieces, (lab_ref, row_ref, left) = rest[:count], rest[count:]
    thick, height, depth = v_ref.shape
    lanes = thick * height
    labels = base_ref.shape[0]
    base = base_of(base_ref)
    terms = affine(base, 0.5)
    devices = slabs * blocks
    x_total = slabs * thick

    row = lax.broadcasted_iota(jnp.int32, (slabs, lanes), 0)
    everywhere = Planes((slabs, lanes), height, thick * row, x_total)
    sums = [None] * (2 * labels)
    for end in range(blocks - 1):
        planes = []
        for beyond, which in ((0, 2), (0, 3), (1, 0), (1, 1)):
            start = (end + beyond) * ROWS + which
            planes.append(
                jnp.concatenate(
                    [
                        got_ref[
                            pl.ds(start + outer * blocks * ROWS, count, stride=groups * blocks * ROWS)
                        ]
                        for outer in range(groups)
                    ],
                    axis=0,
                )
            )
        pulls = [attraction(plane, terms) for plane in planes]
        first = [project_simplex(pull, 0.5) for pull in pulls]
        divergence = [[], []]
        for label in range(labels):
            duals = [
                everywhere.dual(first[index][label], first[index + 1][label])
                for index in range(3)
            ]
            for index in (1, 2):
                x, y, z = duals[index]
                divergence[index - 1].append(
                    everywhere.behind_xy(x, y) + (z - duals[index - 1][2])
                )
        for index in (1, 2):
            entries = [
                first[index][label] + 0.0625 * divergence[index - 1][label] + pulls[index][label]
                for label in range(labels)
            ]
            for label, value in enumerate(project_simplex(entries, 0.5)):
                add_to(sums, label, value)
                add_to(sums, labels + label, value * planes[index])
    parts = got_ref[pl.ds(ROWS - 1, devices, stride=ROWS), :]
    lane = lax.broadcasted_iota(jnp.int32, (1, lanes), 1)
    parts = jnp.sum(parts, axis=0, keepdims=True)
    whole = []
    for index in range(2 * labels):
        part = jnp.where(lane == index, parts, 0.0)
        if blocks > 1:
            part = part + jnp.sum(sums[index], axis=0, keepdims=True)
        whole.append(2.0 * jnp.sum(part, axis=1, keepdims=True))
    centers = [
        (whole[labels + label] + prior_weight * base[label]) / (whole[label] + prior_weight)
        for label in range(labels)
    ]

    row = lax.broadcasted_iota(jnp.int32, (8, lanes), 0)
    local = Planes((8, lanes), height, thick * (slab - 1 + (row & 3)), x_total)
    planes = [q_ref[column] for column in range(6)]
    for which in range(3):
        index = rank_of(jnp.clip(slab - 1 + which, 0, slabs - 1)) * blocks
        low = (index + jnp.maximum(block - 1, 0)) * ROWS
        high = (index + jnp.minimum(block + 1, blocks - 1)) * ROWS
        for column in range(2):
            source = got_ref[pl.ds(low + 2 + column, 1), :]
            planes[column] = jnp.where(row == which, source, planes[column])
            source = got_ref[pl.ds(high + column, 1), :]
            planes[4 + column] = jnp.where(row == 4 + which, source, planes[4 + column])
    pulls = [attraction(plane, terms) for plane in planes]
    first = [project_simplex(pull, 0.5) for pull in pulls]
    duals = []
    for label in range(labels):
        duals.append([])
        for column in range(5):
            x, y, z = local.dual(first[column][label], first[column + 1][label])
            duals[label].append((x * local.inside, y, z))
    second, smooth = {}, {}
    for column in range(1, 5):
        entries = []
        for label in range(labels):
            x, y, z = duals[label][column]
            divergence = local.behind_xy(x, y) + (z - duals[label][column - 1][2])
            entries.append(first[column][label] + 0.0625 * divergence + pulls[column][label])
        second[column] = [value + value for value in project_simplex(entries, 0.5)]
        smooth[column] = [
            second[column][label] - first[column][label] for label in range(labels)
        ]
    for label in range(labels):
        for column in range(1, 4):
            x, y, z = local.dual(
                smooth[column][label], smooth[column + 1][label], duals[label][column]
            )
            duals[label][column] = (x * local.inside, y, z)
    terms = affine(centers, 1.0)
    edge = {}
    for column in (2, 3):
        pull = attraction(planes[column], terms)
        entries = []
        for label in range(labels):
            x, y, z = duals[label][column]
            divergence = local.behind_xy(x, y) + (z - duals[label][column - 1][2])
            entries.append(second[column][label] + 0.125 * divergence + pull[label])
        edge[column] = project_simplex(entries, 1.0)
    step = depth // labels
    tiles = [jnp.zeros((8, lanes), jnp.float32) for _ in range(depth // 8)]
    for label in range(labels):
        two, three = edge[2][label], edge[3][label]
        place = label * step // 8
        tiles[place] = tiles[place] + jnp.where(
            row == 0, pltpu.roll(two, 7, 0), jnp.where(row == 1, three, 0.0)
        )
        place = (place - 1) % (depth // 8)
        tiles[place] = tiles[place] + jnp.where(
            row == 6, pltpu.roll(two, 1, 0), jnp.where(row == 7, pltpu.roll(three, 2, 0), 0.0)
        )
    columns = jnp.transpose(jnp.concatenate(tiles, axis=0))

    z = lax.broadcasted_iota(jnp.int32, (CHUNK, depth), 1)
    replaced = ((z < 2) & (block > 0)) | ((z >= depth - 2) & (block < blocks - 1))
    sums = [None] * (2 * labels)
    for layer in range(thick):
        for start in range(0, height, CHUNK):
            rows = slice(start, start + CHUNK)
            values = v_ref[layer, rows]
            entries = [
                w_ref[label, layer, rows] + pull
                for label, pull in enumerate(attraction(values, terms))
            ]
            for label, value in enumerate(project_simplex(entries, 1.0)):
                column = columns[layer * height + start : layer * height + start + CHUNK]
                if label:
                    column = pltpu.roll(column, depth - label * step, 1)
                value = jnp.where(replaced, column, value)
                lab_ref[label, layer, rows] = value
                add_to(sums, label, value)
                add_to(sums, labels + label, value * values)
    row_ref[...] = jnp.broadcast_to(pack_sums(sums, (1, lanes)), (devices, lanes))
    copy = pltpu.make_async_copy(row_ref, sums_ref, left)
    copy.start()
    rows = height // count
    me = lax.axis_index("gy")
    for other in range(count):
        start = pl.multiple_of((me ^ other) * rows, rows)
        pieces[other][...] = lab_ref[:, :, pl.ds(start, rows), :]
    copy.wait()


def join_kernel(*refs):
    *pieces, out_ref = refs
    me = lax.axis_index("gy")
    thick = pieces[0].shape[1]
    for other, piece in enumerate(pieces):
        out_ref[:, pl.ds((me ^ other) * thick, thick)] = piece[...]


def local(volume, levels):
    slabs = lax.axis_size(SLABS)
    blocks = lax.axis_size("gz")
    count = lax.axis_size("gy")
    devices = slabs * blocks
    thick, height, depth = volume.shape
    labels = levels.shape[0]
    lanes = thick * height
    if thick != 2 or labels != 4 or count & (count - 1):
        raise ValueError("unsupported sizes")
    f32 = functools.partial(jax.ShapeDtypeStruct, dtype=jnp.float32)
    vmem = pl.BlockSpec(memory_space=pltpu.VMEM)

    base_levels = levels.astype(jnp.float32) / 255.0
    params = pltpu.CompilerParams(vmem_limit_bytes=8 << 20)
    base = pl.pallas_call(
        base_kernel,
        out_shape=f32((labels, lanes)),
        in_specs=[vmem],
        out_specs=vmem,
        compiler_params=params,
        cost_estimate=pl.CostEstimate(flops=COVER, bytes_accessed=0, transcendentals=0),
        name="base",
    )(levels.reshape(1, labels))

    pairs = [(i, i ^ 1) for i in range(slabs)]
    across = [(i, (i + 1) % slabs) for i in range(1, slabs, 2)]
    across += [(target, source) for source, target in across]
    pair = lax.ppermute(volume, SLABS, pairs)
    other = lax.ppermute(volume, SLABS, across)

    halves, entries, parts, edges = pl.pallas_call(
        pair_kernel,
        out_shape=[
            f32((labels, thick + 1, height + 8, depth)),
            f32((labels, height, depth)),
            f32((2 * labels, CHUNK, depth)),
            f32((4, lanes)),
        ],
        in_specs=[vmem] * 3,
        out_specs=[vmem] * 4,
        scratch_shapes=[
            pltpu.VMEM((labels, 2, height + 8, depth), jnp.float32),
            pltpu.VMEM((labels, 2, height, depth), jnp.float32),
            pltpu.VMEM((labels, 2, height, depth), jnp.float32),
        ],
        compiler_params=params,
        cost_estimate=pl.CostEstimate(flops=COVER, bytes_accessed=0, transcendentals=0),
        name="pair",
    )(volume, pair, base)
    sent = pl.pallas_call(
        first_kernel,
        out_shape=f32((devices * ROWS, lanes)),
        in_specs=[vmem] * 7,
        out_specs=vmem,
        scratch_shapes=[
            pltpu.VMEM((labels, 2, height + 8, depth), jnp.float32),
            pltpu.VMEM((labels, height + 8, depth), jnp.float32),
        ],
        compiler_params=params,
        name="first",
    )(volume, other, base, halves, entries, parts, edges)
    got = lax.all_to_all(sent.reshape(devices, 1, ROWS * lanes), AXES, 0, 0, tiled=True)
    got = got.reshape(devices * ROWS, lanes)

    layers = 3 * thick
    ahead, planes = pl.pallas_call(
        ahead_kernel,
        out_shape=[f32((labels, thick, height, depth)), f32((6, 8, lanes))],
        in_specs=[vmem] * 4,
        out_specs=[vmem] * 2,
        scratch_shapes=[
            pltpu.VMEM((labels, layers, height + 8, depth), jnp.float32),
            pltpu.VMEM((labels, layers, height + 8, depth), jnp.float32),
            pltpu.VMEM((labels, 3, layers, height, depth), jnp.float32),
            pltpu.VMEM((labels, layers, height + 8, depth), jnp.float32),
            pltpu.VMEM((labels, layers, height, depth), jnp.float32),
        ],
        cost_estimate=pl.CostEstimate(
            flops=200 * labels * layers * height * depth,
            bytes_accessed=4 * 20 * height * depth,
            transcendentals=0,
        ),
        compiler_params=params,
        name="ahead",
    )(volume, pair, other, base)

    piece = f32((labels, thick, height // count, depth))
    sums, *pieces = pl.pallas_call(
        last_kernel,
        out_shape=[f32((devices, lanes))] + [piece] * count,
        in_specs=[vmem] * 5,
        out_specs=[pl.BlockSpec(memory_space=pltpu.HBM)] + [vmem] * count,
        scratch_shapes=[
            pltpu.VMEM((labels, thick, height, depth), jnp.float32),
            pltpu.VMEM((devices, lanes), jnp.float32),
            pltpu.SemaphoreType.DMA,
        ],
        compiler_params=params,
        name="last",
    )(volume, ahead, planes, base, got)

    total = lax.all_to_all(sums.reshape(devices, 1, lanes), AXES, 0, 0, tiled=True)
    for shift in range(1, count):
        pieces[shift] = lax.ppermute(pieces[shift], "gy", [(i, i ^ shift) for i in range(count)])
    join = pl.pallas_call(
        join_kernel,
        out_shape=f32((labels, thick * count, height // count, depth)),
        in_specs=[vmem] * count,
        out_specs=vmem,
        cost_estimate=pl.CostEstimate(
            flops=labels * thick * height * depth,
            bytes_accessed=8 * labels * thick * height * depth,
            transcendentals=0,
        ),
        compiler_params=params,
        name="join",
    )
    labelling = join(*pieces)
    total = total.sum((0, 1))
    sizes_all, weighted_all = total[:labels], total[labels : 2 * labels]
    centers = (weighted_all + prior_weight * base_levels) / (sizes_all + prior_weight)
    return (labelling, centers)


def solution(mesh):
    return jax.shard_map(
        local,
        mesh=mesh,
        in_specs=(P(("gx", "gy"), None, "gz"), P()),
        out_specs=(P(None, "gx", "gy", "gz"), P()),
        check_vma=False,
    )
```
